32 devices in a mesh: outer: 2 (over core), dp: 4 (over z), tensor: 4 (over y, x).
Axes of the slice: x: 2, y: 2, z: 4, core: 2. Of those that a mesh axis runs over, the one named last changes fastest.
Arguments:
- attn: bfloat16 [2048, 8192], P(('outer', 'dp'), 'tensor'), may hold values from -6 to 6
- out_weight: bfloat16 [8192, 8192], P(None, 'tensor'), may hold values from -0.0625 to 0.0625
- resid: bfloat16 [2048, 8192], P(('outer', 'dp'), 'tensor'), may hold values from -8 to 8
- norm_gain: bfloat16 [8192], P('tensor'), may hold values from 0.5 to 1.5
- head: bfloat16 [8192], P('tensor'), may hold values from -1 to 1
- lengths: int32 [32], P(('outer', 'dp')), may hold values from 1 to 64
- pairs: int32 [32, 2], P(('outer', 'dp')), may hold values from 0 to 3, as said below
- pair_valid: int32 [32], P(('outer', 'dp')), may hold values from 0 to 1, as said below
- loss_scale: float32 [1], replicated, may hold values from 1024 to 8192
Outputs:
- loss: float32 [1], replicated
- grad_out_proj: float32 [8192, 8192], P(('outer', 'dp'), 'tensor')
- grad_gain: float32 [8192], P('tensor')
- grad_head: float32 [8192], P('tensor')
The draws below stay inside these ranges and needn't reach their ends.
Inputs may be any that keep to these rules, and one draw needn't show every extreme that they name: `pairs`: in each pair the two numbers differ; the first pair of each replica is valid. `pair_valid`: the first of each replica's 4 entries is 1.
All inputs are finite; a program needn't handle non-finite values.
Results may differ from the reference program's by a relative error of at most 0.003.
Values may be sent and summed in bfloat16 or wider, within the bound.
A program may use at most 128 MiB of HBM per device.

```python
import math
import jax
import jax.numpy as jnp
from jax import lax

D = 8192
SEQ_LEN = 64
SEQS_DEV = 4
PAIRS_DEV = 4
HD = 8192
SEQS = 32
TOKENS = 2048
PAIRS = 32


def head_vector(key):
    values = jax.random.normal(jax.random.fold_in(key, 41), (D,), jnp.float32) * (D // 16) ** (-0.5)
    return jnp.clip(values, -1.0, 1.0)


def draw_head(key, part):
    return head_vector(key).astype(jnp.bfloat16)


def draw_pairs(key, part):
    first = jax.random.randint(jax.random.fold_in(key, 11), (PAIRS,), 0, SEQS_DEV)
    step = jax.random.randint(jax.random.fold_in(key, 12), (PAIRS,), 1, SEQS_DEV)
    second = (first + step) % SEQS_DEV
    return jnp.stack([first, second], axis=1).astype(jnp.int32)


def draw_pair_valid(key, part):
    coin = jax.random.randint(jax.random.fold_in(key, 21), (PAIRS,), 0, 4)
    leading = jnp.arange(PAIRS) % PAIRS_DEV == 0
    return jnp.where(leading | (coin > 0), 1, 0).astype(jnp.int32)


def draw_resid(key, part):
    headv = head_vector(key)
    unit = headv * D ** 0.5 / jnp.sqrt(jnp.sum(headv * headv))
    rising = 0.5 * jnp.exp(jnp.log(4.0) * jnp.arange(D, dtype=jnp.float32) / D)
    rough = jax.random.uniform(jax.random.fold_in(key, 31), (D,), jnp.float32, 0.7, 1.4)
    shape = rising * rough
    base_var = jnp.mean(shape * shape)
    base = jax.random.normal(jax.random.fold_in(key, 34), (TOKENS, D), jnp.float32)
    rest = base * shape[None, :]
    spread = (base_var + 1.0) * jnp.ones((TOKENS, 1), jnp.float32)
    share = 0.3
    along = share / (1.0 - share * share) ** 0.5 * jnp.sqrt(spread)
    values = rest + along * unit[None, :]
    return jnp.clip(values, -8.0, 8.0).astype(jnp.bfloat16)


def plant(values, rng, least, high):
    longest = values.shape.index(max(values.shape))
    spots = []
    for shift in (0, 1):
        where = [jax.random.randint(jax.random.fold_in(rng, axis), (), 0, length) for axis, length in enumerate(values.shape)]
        where[longest] = (where[longest] + shift) % values.shape[longest]
        spots.append(tuple(where))
    return values.at[spots[0]].set(least).at[spots[1]].set(high)


def levels(rng, extent, shards, least, top_value):
    level, own = 1.0, jax.random.fold_in(rng, 6)
    for dim, parts in shards:
        steps = jnp.exp(jax.random.uniform(jax.random.fold_in(own, dim), (parts,), jnp.float32, least / len(shards), top_value / len(shards)))
        level = level * jnp.repeat(steps, extent[dim] // parts).reshape([-1 if axis == dim else 1 for axis in range(len(extent))])
    return level


def noise(own_key, extent, width, limit, split=(), kind=jnp.bfloat16):
    values = jax.random.normal(own_key, extent, jnp.float32) * width
    if len(split) > 0:
        values = levels(own_key, extent, split, -0.22, 0.18) * values
    return jnp.clip(values, min=-limit, max=limit).astype(kind)


def setup_inputs(seed: int = 0) -> dict:
    keys = jax.random.split(jax.random.key(seed), 10)
    attn = noise(keys[0], (TOKENS, HD), 1.0, 6.0, ((0, 8), (1, 4)))
    out_weight = noise(keys[1], (D, HD), HD ** -0.5, 0.0625, ((1, 4),))
    resid = draw_resid(jax.random.fold_in(keys[9], 71), 0)
    norm_gain = jnp.clip(1.0 + 0.1 * jax.random.normal(keys[3], (D,), jnp.float32), 0.5, 1.5).astype(jnp.bfloat16)
    head = draw_head(jax.random.fold_in(keys[9], 71), 0)
    lengths = plant(jax.random.randint(keys[5], (SEQS,), 1, SEQ_LEN + 1), jax.random.fold_in(keys[5], 1), 1, SEQ_LEN).astype(jnp.int32)
    pairs = draw_pairs(jax.random.fold_in(keys[9], 71), 0)
    pair_valid = draw_pair_valid(jax.random.fold_in(keys[9], 71), 0)
    loss_scale = jnp.clip(jnp.exp(jax.random.uniform(keys[8], (1,), jnp.float32, math.log(1024.0), math.log(8192.0))), 1024.0, 8192.0)
    return {"attn": attn, "out_weight": out_weight, "resid": resid, "norm_gain": norm_gain, "head": head, "lengths": lengths, "pairs": pairs, "pair_valid": pair_valid, "loss_scale": loss_scale}


def reference(attn, out_weight, resid, norm_gain, head, lengths, pairs, pair_valid, loss_scale):
    f32 = jnp.float32
    attn_f = attn.astype(f32)
    proj = jnp.dot(attn_f, out_weight.astype(f32).T)
    z = resid.astype(f32) + proj
    gain = norm_gain.astype(f32)
    headv = head.astype(f32)
    inv = 1.0 / jnp.sqrt(lax.optimization_barrier(jnp.mean(z * z, axis=1, keepdims=True)) + 1e-05)
    normed = z * inv * gain
    score = lax.optimization_barrier(jnp.sum(normed * headv, axis=1))
    live = (jnp.arange(SEQ_LEN)[None, :] < lengths[:, None]).astype(f32)
    lens = lengths.astype(f32)
    reward = lax.optimization_barrier(jnp.sum(score.reshape(SEQS, SEQ_LEN) * live, axis=1)) / lens
    offset = (jnp.arange(PAIRS) // PAIRS_DEV * SEQS_DEV).astype(jnp.int32)
    chosen = pairs[:, 0] + offset
    rejected = pairs[:, 1] + offset
    valid = pair_valid.astype(f32)
    margin = reward[chosen] - reward[rejected]
    count = jnp.sum(valid)
    loss = jnp.sum(valid * jax.nn.softplus(-margin)) / count
    dmargin = -loss_scale[0] * valid * jax.nn.sigmoid(-margin) / count
    dreward = jnp.zeros((SEQS,), f32).at[chosen].add(dmargin).at[rejected].add(-dmargin)
    dscore = ((dreward / lens)[:, None] * live).reshape(TOKENS)
    grad_head = lax.optimization_barrier(jnp.sum(dscore[:, None] * normed, axis=0))
    grad_gain = lax.optimization_barrier(jnp.sum(dscore[:, None] * headv * z * inv, axis=0))
    a = dscore[:, None] * headv * gain
    dproj = inv * a - z * inv ** 3 * lax.optimization_barrier(jnp.sum(a * z, axis=1, keepdims=True)) / D
    dproj = dproj.astype(jnp.bfloat16)
    grad_out_proj = jnp.dot(dproj.astype(f32).T, attn_f)
    return (loss.reshape(1), grad_out_proj, grad_gain, grad_head)
```

```python
import functools

import jax
import jax.numpy as jnp
from jax import lax
from jax.experimental import pallas as pl
from jax.experimental.pallas import tpu as pltpu
from jax.sharding import PartitionSpec as P

MESH = pl.DeviceIdType.MESH
F32 = jnp.float32
BF16 = jnp.bfloat16
SLOTS = 3


def bits_of(count):
    return count.bit_length() - 1


def flip(index, mask, bits):
    out = 0
    for j in range(bits):
        out = out + ((index // 2**j + mask // 2**j) % 2) * 2**j
    return out


def reverse(index, bits):
    out = 0
    for j in range(bits):
        out = out + ((index // 2**j) % 2) * 2 ** (bits - 1 - j)
    return out


def kernel(
    sizes,
    attn,
    weight,
    resid,
    gain,
    headv,
    lengths,
    pairs,
    pair_valid,
    loss_scale,
    grad,
    ggain,
    ghead,
    loss_out,
    exch,
    attn_all,
    wbuf,
    attn_t,
    res_t,
    vbuf,
    part,
    got,
    keep,
    dp,
    bsrc,
    ball,
    bcol,
    hacc,
    stat,
    stat_in,
    csrc,
    cin,
    lsrc,
    lin,
    qsrc,
    qin,
    qsum,
    qall,
    wsem,
    rs_send,
    rs_recv,
    b_send,
    b_recv,
    st_send,
    st_recv,
    c_send,
    c_recv,
    l_send,
    l_recv,
    q_send,
    q_recv,
    t_send,
    t_recv,
    ag_local,
    ag_right,
    ag_left,
    ag_out,
    ag_recv,
    z_send,
    z_recv,
    e_send,
    e_recv,
):
    T, O, Z = sizes
    N = O * Z
    bits = bits_of(T)
    R = N // T
    half = T // 2
    tok, feats = resid.shape
    width = feats * T
    blk = width // N
    q = blk // T
    h = q // 2
    K = (N // 2) * h
    steps = 4 * T
    o, p, t = lax.axis_index("outer"), lax.axis_index("dp"), lax.axis_index("tensor")
    me = o * Z + p

    def replica(k):
        return (k // Z, k % Z, t)

    def rank(r):
        return (o, p, r)

    barrier = pltpu.get_barrier_semaphore()
    for r in range(1, T):
        pl.semaphore_signal(barrier, inc=1, device_id=rank(flip(t, r, bits)), device_id_type=MESH)
    for d in range(1, N):
        pl.semaphore_signal(barrier, inc=1, device_id=replica((me + d) % N), device_id_type=MESH)

    def piece_of(i):
        e, g = i // 2, i % 2
        s = e % 2
        j = T - 1 - e // 2
        return s, j, g

    def target(s, j):
        return flip(t, s * j + (1 - s) * reverse(j, bits), bits)

    def load(i):
        s, j, g = piece_of(i)
        return pltpu.make_async_copy(
            weight.at[pl.ds(g * (N // 2), N // 2), target(s, j) * 2 + s],
            wbuf.at[i % SLOTS],
            wsem.at[i % SLOTS],
        )

    for i in range(min(SLOTS - 1, steps)):
        load(i).start()

    both = gain[...] * headv[...]
    for r in range(T):
        for s in range(2):
            for b in range(R):
                start = b * blk + r * q + s * h
                bsrc[r * 2 + s, 0:1, b * h : (b + 1) * h] = both[:, start : start + h]
    ball[t] = bsrc[...]
    valid = pair_valid[...].astype(F32)
    csrc[...] = jnp.broadcast_to(jnp.sum(valid, axis=1, keepdims=True), csrc.shape)

    def turn_attn(c, carry):
        cols = pl.ds(pl.multiple_of(c * 128, 128), 128)
        attn_t[cols, :] = attn[:, cols].astype(F32).T.astype(BF16)
        return carry

    lax.fori_loop(0, attn.shape[1] // 128, turn_attn, 0)
    pl.semaphore_wait(barrier, T - 1 + N - 1)

    def peer_copy(src, dst, send, recv, d):
        return pltpu.make_async_remote_copy(
            src_ref=src,
            dst_ref=dst.at[d],
            send_sem=send.at[d],
            recv_sem=recv.at[d],
            device_id=replica((me + d) % N),
            device_id_type=MESH,
        )

    def rank_copy(src, dst, send, recv, r):
        return pltpu.make_async_remote_copy(
            src_ref=src,
            dst_ref=dst,
            send_sem=send.at[r],
            recv_sem=recv.at[r],
            device_id=rank(flip(t, r, bits)),
            device_id_type=MESH,
        )

    def both_copy(r):
        return rank_copy(bsrc, ball.at[t], b_send, b_recv, r)

    for r in range(1, T):
        both_copy(r).start()

    def block_rows(outer, b):
        return outer * Z + b

    def ag_copy(src, b, send, where):
        return pltpu.make_async_remote_copy(
            src_ref=src,
            dst_ref=attn_all.at[block_rows(o, b)],
            send_sem=send,
            recv_sem=ag_recv.at[o, b],
            device_id=where,
            device_id_type=MESH,
        )

    def right_copy(s):
        b = (p + Z - s) % Z
        src = attn if s == 0 else attn_all.at[block_rows(o, b)]
        return ag_copy(src, b, ag_right.at[s], (o, (p + 1) % Z, t))

    def left_copy(s):
        b = (p + s) % Z
        src = attn if s == 0 else attn_all.at[block_rows(o, b)]
        return ag_copy(src, b, ag_left.at[s], (o, (p + Z - 1) % Z, t))

    def right_sends(s):
        return (p >= s) & (p < Z - 1)

    def left_sends(s):
        return (p + s < Z) & (p > 0)

    def out_copy(b, e, own=False):
        src = attn if own else attn_all.at[block_rows(o, b)]
        return ag_copy(src, b, ag_out.at[e, b], ((o + e) % O, p, t))

    def arrived(outer, b):
        rows = attn_all.at[block_rows(outer, b)]
        return pltpu.make_async_remote_copy(
            src_ref=rows,
            dst_ref=rows,
            send_sem=ag_out.at[0, 0],
            recv_sem=ag_recv.at[outer, b],
            device_id=(o, (p + 1) % Z, t),
            device_id_type=MESH,
        )

    def arrival(s):
        for ok, b in ((p - 1 - s >= 0, (p + Z - 1 - s) % Z), (p + 1 + s < Z, (p + 1 + s) % Z)):

            @pl.when(ok)
            def _():
                arrived(o, b).wait_recv()
                for e in range(1, O):
                    out_copy(b, e).start()

        if s + 1 < Z - 1:
            for ok, copy in ((right_sends(s + 1), right_copy), (left_sends(s + 1), left_copy)):

                @pl.when(ok)
                def _():
                    copy(s + 1).start()

    for ok, copy in ((right_sends(0), right_copy), (left_sends(0), left_copy)):

        @pl.when(ok)
        def _():
            copy(0).start()

    for e in range(1, O):
        out_copy(p, e, True).start()
    own_rows = pltpu.make_async_copy(attn, attn_all.at[block_rows(o, p)], ag_local)
    own_rows.start()
    for d in range(1, N):
        peer_copy(csrc, cin, c_send, c_recv, d).start()

    def turn_resid(c, carry):
        cols = pl.ds(pl.multiple_of(c * 128, 128), 128)
        res_t[cols, :] = resid[:, cols].astype(F32).T.astype(BF16)
        return carry

    lax.fori_loop(0, feats // 128, turn_resid, 0)
    hacc[...] = jnp.zeros_like(hacc)
    for r in range(1, T):
        both_copy(r).wait_recv()

    def rs_copy(s, j, g, mask):
        return pltpu.make_async_remote_copy(
            src_ref=part.at[s, j, g],
            dst_ref=got.at[s, j, g],
            send_sem=rs_send.at[s, j, g],
            recv_sem=rs_recv.at[s, j, g],
            device_id=rank(flip(t, mask, bits)),
            device_id_type=MESH,
        )

    def rs_mask(s, b):
        return s * 2**b + (1 - s) * 2 ** (bits - 1 - b)

    row16 = lax.broadcasted_iota(jnp.int32, (16, R * h), 0)

    def thirds(row):
        first = row.astype(BF16).astype(F32)
        second = (row - first).astype(BF16).astype(F32)
        third = row - first - second
        rows = jnp.where(row16 == 0, first, jnp.where(row16 == 1, second, third))
        return jnp.where(row16 < 3, rows, 0.0).astype(BF16)

    def project(i, carry):
        @pl.when(i + SLOTS - 1 < steps)
        def _():
            load(i + SLOTS - 1).start()

        load(i).wait()
        s, j, g = piece_of(i)
        r = target(s, j)
        vbuf[...] = jnp.dot(
            wbuf[i % SLOTS].reshape(K, wbuf.shape[3]), attn_t[...], preferred_element_type=F32
        )

        @pl.when(t // half == g)
        def _():
            for b in range(R):
                rows = pl.ds(pl.multiple_of(((t % half) * R + b) * h, h), h)
                mine = pl.ds(pl.multiple_of(b * blk + (r * 2 + s) * h, h), h)
                vbuf[rows, :] = vbuf[rows, :] + res_t[mine, :].astype(F32)

        total = hacc[...]
        for n in range(half):
            lhs = thirds(ball[g * half + n, r * 2 + s])
            rows = vbuf[n * R * h : (n + 1) * R * h, :]
            high = rows.astype(BF16)
            low = (rows - high.astype(F32)).astype(BF16)
            total = total + jnp.dot(lhs, high, preferred_element_type=F32)
            total = total + jnp.dot(lhs, low, preferred_element_type=F32)
        hacc[...] = total

        @pl.when(j >= half)
        def _():
            part[s, j, g] = vbuf[...].astype(BF16)
            rs_copy(s, j, g, rs_mask(s, bits - 1)).start()

        @pl.when(j < half)
        def _():
            keep[s, j % half, g] = vbuf[...]

        return carry

    lax.fori_loop(0, steps, project, 0)

    for b in range(bits - 2, -1, -1):

        def combine(x, carry, b=b):
            j, s, g = 2**b + x // 4, x % 2, (x // 2) % 2
            total = keep[s, j, g]
            for up in range(b + 1, bits):
                rs_copy(s, j + 2**up, g, rs_mask(s, up)).wait_recv()
                total = total + got[s, j + 2**up, g].astype(F32)
            part[s, j, g] = total.astype(BF16)
            rs_copy(s, j, g, rs_mask(s, b)).start()
            return carry

        lax.fori_loop(0, 4 * 2**b, combine, 0)

    arrival(0)

    def clear(j, carry):
        grad[pl.ds(pl.multiple_of(j * 128, 128), 128), :] = jnp.zeros((128, grad.shape[1]), F32)
        return carry

    lax.fori_loop(0, blk // 128, clear, 0)
    span = R * h
    diag = lax.broadcasted_iota(jnp.int32, (span, span), 0) == lax.broadcasted_iota(
        jnp.int32, (span, span), 1
    )

    def columns(x, carry):
        s, n = x % 2, x // 2
        row = jnp.broadcast_to(ball[n, t * 2 + s], (span, span))
        col = jnp.sum(jnp.where(diag, row, 0.0), axis=1, keepdims=True)
        rows = pl.ds(pl.multiple_of((n % half) * span, span), span)
        bcol[s, n // half, rows, :] = jnp.broadcast_to(col, (span, 128))
        return carry

    lax.fori_loop(0, 2 * T, columns, 0)

    S = lengths.shape[1]
    lens = lengths[...].astype(F32)
    same = lax.broadcasted_iota(jnp.int32, (S, S), 0) == lax.broadcasted_iota(jnp.int32, (S, S), 1)
    lens = jnp.sum(jnp.where(same, jnp.broadcast_to(lens, (S, S)), 0.0), axis=1, keepdims=True)
    seq_len = tok // S
    slot = lax.broadcasted_iota(jnp.int32, (S, tok), 1) - seq_len * lax.broadcasted_iota(
        jnp.int32, (S, tok), 0
    )
    live = (slot >= 0) & (slot.astype(F32) < lens)
    pool = jnp.where(live, 1.0 / lens, 0.0)
    who = lax.broadcasted_iota(jnp.int32, (S, pairs.shape[1]), 0)
    select = jnp.where(who == pairs[0:1, :], 1.0, 0.0) - jnp.where(who == pairs[1:2, :], 1.0, 0.0)

    def final(x, squares):
        s, g = x % 2, x // 2
        total = keep[s, 0, g]
        for up in range(bits - 1, -1, -1):
            rs_copy(s, 2**up, g, rs_mask(s, up)).wait_recv()
            total = total + got[s, 2**up, g].astype(F32)
        keep[s, 0, g] = total
        return squares + jnp.sum(total * total, axis=0, keepdims=True)

    squares = lax.fori_loop(0, 4, final, jnp.zeros((1, tok), F32))
    heads = jnp.sum(hacc[...], axis=0, keepdims=True)
    stat[0:1, :] = squares
    stat[1:2, :] = heads

    def stat_copy(r):
        return rank_copy(stat, stat_in.at[r], st_send, st_recv, r)

    for r in range(1, T):
        stat_copy(r).start()
    count = csrc[0:1, 0:1]
    for d in range(1, N):
        peer_copy(csrc, cin, c_send, c_recv, d).wait_recv()
        count = count + cin[d, 0:1, 0:1]
    for r in range(1, T):
        stat_copy(r).wait_recv()
        squares = squares + stat_in[r, 0:1, :]
        heads = heads + stat_in[r, 1:2, :]
    inv = 1.0 / jnp.sqrt(squares / width + 1e-05)
    score = heads * inv
    reward = jnp.sum(pool * score, axis=1, keepdims=True)
    margin = jnp.sum(select * reward, axis=0, keepdims=True)
    soft = jnp.maximum(-margin, 0.0) + jnp.log1p(jnp.exp(-jnp.abs(margin)))
    loss = jnp.sum(valid * soft, axis=1, keepdims=True)
    dmargin = -loss_scale[...] * valid * jax.nn.sigmoid(-margin) / count
    dreward = jnp.sum(select * dmargin, axis=1, keepdims=True)
    dscore = jnp.sum(pool * dreward, axis=0, keepdims=True)
    scale = inv * dscore
    pull = inv * inv * inv * dscore * heads / width

    def make_dproj(x, carry):
        s, g, n = x % 2, x // N, (x // 2) % (N // 2)
        rows = pl.ds(pl.multiple_of(n * h, h), h)
        spot = pl.ds(pl.multiple_of(s * h, h), h)
        for c in range(tok // 128):
            cols = slice(c * 128, (c + 1) * 128)
            dp[g * (N // 2) + n, spot, cols] = (
                scale[:, cols] * bcol[s, g, rows, :] - keep[s, 0, g, rows, cols] * pull[:, cols]
            ).astype(BF16)
        return carry

    lax.fori_loop(0, 2 * N, make_dproj, 0)

    side = p // (Z - Z // 2)
    edge = side * (Z - 1 - p) + (1 - side) * p

    def place(i):
        n = i // O
        past = (n + Z - 1 - edge) // Z
        spot = past * n + (1 - past) * (edge - n)
        return ((o + i) % O) * Z + side * (Z - 1 - spot) + (1 - side) * spot

    def slot_rows(r):
        return pl.ds(pl.multiple_of(r * q, q), q)

    def piece_copy(k):
        return pltpu.make_async_remote_copy(
            src_ref=dp.at[k],
            dst_ref=exch.at[me, slot_rows(t)],
            send_sem=z_send.at[k],
            recv_sem=z_recv.at[me],
            device_id=replica(k),
            device_id_type=MESH,
        )

    def piece_arrived(k):
        rows = exch.at[k, slot_rows(t)]
        return pltpu.make_async_remote_copy(
            src_ref=rows,
            dst_ref=rows,
            send_sem=z_send.at[k],
            recv_sem=z_recv.at[k],
            device_id=replica((me + 1) % N),
            device_id_type=MESH,
        )

    own_piece = pltpu.make_async_copy(dp.at[me], exch.at[me, slot_rows(t)], z_recv.at[me])
    own_piece.start()

    def send_piece(i, carry):
        piece_copy(place(i)).start()
        return carry

    lax.fori_loop(1, N, send_piece, 0)

    lsrc[...] = jnp.broadcast_to(loss, lsrc.shape)
    for s in range(2):
        for g in range(2):
            zw = keep[s, 0, g] * scale
            lanes = zw[:, 0:128]
            for c in range(1, tok // 128):
                lanes = lanes + zw[:, c * 128 : (c + 1) * 128]
            qsrc[s * 2 + g] = jnp.sum(lanes.T, axis=0, keepdims=True)
    for d in range(1, N):
        peer_copy(lsrc, lin, l_send, l_recv, d).start()
        peer_copy(qsrc, qin, q_send, q_recv, d).start()

    def ag_mask(s, b):
        return 2**b if s == 0 else 2 ** (bits - 1 - b)

    def held(s, c):
        return flip(t, c if s == 0 else reverse(c, bits), bits)

    def half_rows(r, s):
        return pl.ds(pl.multiple_of((r * 2 + s) * h, h), h)

    def spread_copy(k, s, c, b):
        rows = exch.at[k, half_rows(held(s, c), s)]
        return pltpu.make_async_remote_copy(
            src_ref=rows,
            dst_ref=rows,
            send_sem=e_send.at[k, s, c + 2**b],
            recv_sem=e_recv.at[k, s, c + 2**b],
            device_id=rank(flip(t, ag_mask(s, b), bits)),
            device_id_type=MESH,
        )

    def spread_arrived(k, s, c):
        rows = exch.at[k, half_rows(held(s, c), s)]
        return pltpu.make_async_remote_copy(
            src_ref=rows,
            dst_ref=rows,
            send_sem=e_send.at[k, s, c],
            recv_sem=e_recv.at[k, s, c],
            device_id=rank(flip(t, 1, bits)),
            device_id_type=MESH,
        )

    def begin(i):
        k = place(i)

        @pl.when(k == me)
        def _():
            own_piece.wait()

        @pl.when(k != me)
        def _():
            piece_arrived(k).wait_recv()

        for b in range(bits):
            for s in range(2):
                spread_copy(k, s, 0, b).start()

    def relay(i):
        k = place(i)
        for b in range(bits - 1):
            for c in range(2**b, 2 ** (b + 1)):
                for s in range(2):
                    spread_arrived(k, s, c).wait_recv()
                    for up in range(b + 1, bits):
                        spread_copy(k, s, c, up).start()

    wide = min(512, grad.shape[1])
    strips = grad.shape[1] // wide

    def multiply(i):
        k = place(i)
        outer, b = k // Z, k % Z
        for c in range(half, T):
            for s in range(2):
                spread_arrived(k, s, c).wait_recv()

        @pl.when(outer != o)
        def _():
            arrived(outer, b).wait_recv()

        def one(c, carry):
            cols = pl.ds(pl.multiple_of(c * wide, wide), wide)
            grad[:, cols] += jnp.dot(exch[k], attn_all[k, :, cols], preferred_element_type=F32)
            return carry

        lax.fori_loop(0, strips, one, 0)

    def gather_q():
        total = qsrc[...]
        for d in range(1, N):
            peer_copy(qsrc, qin, q_send, q_recv, d).wait_recv()
            total = total + qin[d]
        qsum[...] = total
        qall[t] = total
        for r in range(1, T):
            rank_copy(qsum, qall.at[t], t_send, t_recv, r).start()

    def finish_q():
        ltotal = lsrc[...]
        for d in range(1, N):
            peer_copy(lsrc, lin, l_send, l_recv, d).wait_recv()
            ltotal = ltotal + lin[d]
        loss_out[...] = ltotal[0:1, 0:1] / count
        for r in range(1, T):
            rank_copy(qsum, qall.at[t], t_send, t_recv, r).wait_recv()
        for r in range(T):
            for s in range(2):
                for b in range(R):
                    value = jnp.zeros((1, h), F32)
                    for owner in range(T):
                        n = (owner % half) * R + b
                        row = qall[r, s * 2 + owner // half]
                        value = jnp.where(t == owner, row[:, n * h : (n + 1) * h], value)
                    cols = slice(b * blk + r * q + s * h, b * blk + r * q + (s + 1) * h)
                    ggain[:, cols] = value * headv[:, cols]
                    ghead[:, cols] = value * gain[:, cols]

    own_rows.wait()

    def stage(i, carry):
        @pl.when(i < N)
        def _():
            begin(i)

        @pl.when((i >= 1) & (i < N + 1))
        def _():
            relay(i - 1)

        for s in range(1, Z - 1):

            @pl.when(i == min(2 + (s - 1) * O, N))
            def _():
                arrival(s)

        @pl.when(i == N // 2 + 1)
        def _():
            gather_q()

        @pl.when(i == N)
        def _():
            finish_q()

        @pl.when(i >= 2)
        def _():
            multiply(i - 2)

        return carry

    lax.fori_loop(0, N + 2, stage, 0)

    for s in range(Z - 1):
        for ok, copy in ((right_sends(s), right_copy), (left_sends(s), left_copy)):

            @pl.when(ok)
            def _():
                copy(s).wait_send()

    for e in range(1, O):
        for b in range(Z):
            out_copy(b, e).wait_send()
    for d in range(1, N):
        peer_copy(csrc, cin, c_send, c_recv, d).wait_send()
        peer_copy(lsrc, lin, l_send, l_recv, d).wait_send()
        peer_copy(qsrc, qin, q_send, q_recv, d).wait_send()
    for r in range(1, T):
        both_copy(r).wait_send()
        stat_copy(r).wait_send()
        rank_copy(qsum, qall.at[t], t_send, t_recv, r).wait_send()

    def rs_end(x, carry):
        s, g, j = x % 2, (x // 2) % 2, 1 + x // 4
        rs_copy(s, j, g, 1).wait_send()
        return carry

    lax.fori_loop(0, 4 * (T - 1), rs_end, 0)

    def send_end(i, carry):
        piece_copy(place(i)).wait_send()
        return carry

    lax.fori_loop(1, N, send_end, 0)

    def spread_end(k, carry):
        for b in range(bits):
            for c in range(2**b):
                for s in range(2):
                    spread_copy(k, s, c, b).wait_send()
        return carry

    lax.fori_loop(0, N, spread_end, 0)


def shards(sizes, attn, out_weight, resid, norm_gain, head, lengths, pairs, pair_valid, loss_scale):
    T, O, Z = sizes
    N = O * Z
    tok, feats = resid.shape
    width = feats * T
    blk = width // N
    q = blk // T
    h = q // 2
    K = (N // 2) * h
    R = N // T
    heads_dev = attn.shape[1]
    vmem = pl.BlockSpec(memory_space=pltpu.VMEM)
    anyw = pl.BlockSpec(memory_space=pl.ANY)
    sem = pltpu.SemaphoreType.DMA
    bits = bits_of(T)
    grad_out_proj, grad_gain, grad_head, loss = pl.pallas_call(
        functools.partial(kernel, sizes),
        out_shape=(
            pltpu.VMEM((blk, heads_dev), F32),
            jax.ShapeDtypeStruct((1, feats), F32),
            jax.ShapeDtypeStruct((1, feats), F32),
            jax.ShapeDtypeStruct((1, 1), F32),
        ),
        in_specs=[vmem, anyw] + [vmem] * 7,
        out_specs=(vmem, vmem, vmem, vmem),
        scratch_shapes=[
            pltpu.VMEM((N, blk, tok), BF16),
            pltpu.VMEM((N, tok, heads_dev), BF16),
            pltpu.VMEM((SLOTS, N // 2, h, heads_dev), BF16),
            pltpu.VMEM((heads_dev, tok), BF16),
            pltpu.VMEM((feats, tok), BF16),
            pltpu.VMEM((K, tok), F32),
            pltpu.VMEM((2, T, 2, K, tok), BF16),
            pltpu.VMEM((2, T, 2, K, tok), BF16),
            pltpu.VMEM((2, T // 2, 2, K, tok), F32),
            pltpu.VMEM((N, q, tok), BF16),
            pltpu.VMEM((2 * T, 1, R * h), F32),
            pltpu.VMEM((T, 2 * T, 1, R * h), F32),
            pltpu.VMEM((2, 2, K, 128), F32),
            pltpu.VMEM((16, tok), F32),
            pltpu.VMEM((2, tok), F32),
            pltpu.VMEM((T, 2, tok), F32),
            pltpu.VMEM((8, 128), F32),
            pltpu.VMEM((N, 8, 128), F32),
            pltpu.VMEM((8, 128), F32),
            pltpu.VMEM((N, 8, 128), F32),
            pltpu.VMEM((4, 1, K), F32),
            pltpu.VMEM((N, 4, 1, K), F32),
            pltpu.VMEM((4, 1, K), F32),
            pltpu.VMEM((T, 4, 1, K), F32),
            sem((SLOTS,)),
            sem((2, T, 2)),
            sem((2, T, 2)),
            sem((T,)),
            sem((T,)),
            sem((T,)),
            sem((T,)),
            sem((N,)),
            sem((N,)),
            sem((N,)),
            sem((N,)),
            sem((N,)),
            sem((N,)),
            sem((T,)),
            sem((T,)),
            sem,
            sem((Z,)),
            sem((Z,)),
            sem((O, Z)),
            sem((O, Z)),
            sem((N,)),
            sem((N,)),
            sem((N, 2, T)),
            sem((N, 2, T)),
        ],
        compiler_params=pltpu.CompilerParams(
            collective_id=0, has_side_effects=True, vmem_limit_bytes=50 * 1024 * 1024
        ),
    )(
        attn,
        out_weight.reshape(N, 2 * T, h, heads_dev),
        resid,
        norm_gain.astype(F32)[None, :],
        head.astype(F32)[None, :],
        lengths[None, :],
        pairs.T,
        pair_valid[None, :],
        loss_scale[None, :],
    )
    return (loss.reshape(1), grad_out_proj, grad_gain[0], grad_head[0])


def solution(mesh):
    sizes = (mesh.shape["tensor"], mesh.shape["outer"], mesh.shape["dp"])
    return jax.shard_map(
        functools.partial(shards, sizes),
        mesh=mesh,
        in_specs=(
            P(("outer", "dp"), "tensor"),
            P(None, "tensor"),
            P(("outer", "dp"), "tensor"),
            P("tensor"),
            P("tensor"),
            P(("outer", "dp")),
            P(("outer", "dp"), None),
            P(("outer", "dp")),
            P(),
        ),
        out_specs=(P(), P(("outer", "dp"), "tensor"), P("tensor"), P("tensor")),
        check_vma=False,
    )
```

```python
import functools

import jax
import jax.numpy as jnp
from jax import lax
from jax.experimental import pallas as pl
from jax.experimental.pallas import tpu as pltpu
from jax.sharding import PartitionSpec as P

MESH = pl.DeviceIdType.MESH
F32 = jnp.float32
BF16 = jnp.bfloat16
SLOTS = 5


def bits_of(count):
    return count.bit_length() - 1


def flip(index, mask, bits):
    out = 0
    for j in range(bits):
        out = out + ((index // 2**j + mask // 2**j) % 2) * 2**j
    return out


def reverse(index, bits):
    out = 0
    for j in range(bits):
        out = out + ((index // 2**j) % 2) * 2 ** (bits - 1 - j)
    return out


def kernel(
    sizes,
    attn,
    weight,
    resid,
    gain_in,
    head_in,
    lengths,
    pairs,
    pair_valid,
    loss_scale,
    grad,
    ggain,
    ghead,
    loss_out,
    exch,
    attn_all,
    wbuf,
    attn_t,
    res_v,
    res_t,
    gain,
    headv,
    vbuf,
    part,
    got,
    keep,
    dp,
    bsrc,
    ball,
    bcol,
    hacc,
    stat,
    stat_in,
    csrc,
    cin,
    lsrc,
    lin,
    qsrc,
    qin,
    qsum,
    qall,
    wsem,
    rs_send,
    rs_recv,
    b_send,
    b_recv,
    st_send,
    st_recv,
    c_send,
    c_recv,
    l_send,
    l_recv,
    q_send,
    q_recv,
    t_send,
    t_recv,
    ag_local,
    r_local,
    ag_right,
    ag_left,
    ag_out,
    ag_recv,
    z_send,
    z_recv,
    e_send,
    e_recv,
):
    T, O, Z = sizes
    N = O * Z
    bits = bits_of(T)
    R = N // T
    half = T // 2
    tok, feats = resid.shape
    width = feats * T
    blk = width // N
    q = blk // T
    h = q // 2
    K = (N // 2) * h
    steps = 4 * T
    strips, wide = attn_all.shape[1], attn_all.shape[3]
    o, p, t = lax.axis_index("outer"), lax.axis_index("dp"), lax.axis_index("tensor")
    me = o * Z + p

    def replica(k):
        return (k // Z, k % Z, t)

    def rank(r):
        return (o, p, r)

    barrier = pltpu.get_barrier_semaphore()
    for r in range(1, T):
        pl.semaphore_signal(barrier, inc=1, device_id=rank(flip(t, r, bits)), device_id_type=MESH)
    for d in range(1, N):
        pl.semaphore_signal(barrier, inc=1, device_id=replica((me + d) % N), device_id_type=MESH)

    def piece_of(i):
        e, g = i // 2, i % 2
        s = e % 2
        j = T - 1 - e // 2
        return s, j, g

    def target(s, j):
        return flip(t, s * j + (1 - s) * reverse(j, bits), bits)

    def load(i):
        s, j, g = piece_of(i)
        return pltpu.make_async_copy(
            weight.at[pl.ds(g * (N // 2), N // 2), target(s, j) * 2 + s],
            wbuf.at[i % SLOTS],
            wsem.at[i % SLOTS],
        )

    def strip(c):
        return pl.ds(pl.multiple_of(c * wide, wide), wide)

    def own_copy(c):
        return pltpu.make_async_copy(attn.at[:, strip(c)], attn_all.at[me, c], ag_local.at[c])

    resid_copy = pltpu.make_async_copy(resid, res_v, r_local)
    for c in range(strips):
        own_copy(c).start()
    load(0).start()
    resid_copy.start()
    for i in range(1, min(SLOTS - 1, steps)):
        load(i).start()

    lanes = gain_in.shape[1]
    for c in range(feats // lanes):
        gain[:, c * lanes : (c + 1) * lanes] = gain_in[c : c + 1, :].astype(F32)
        headv[:, c * lanes : (c + 1) * lanes] = head_in[c : c + 1, :].astype(F32)
    both = gain[...] * headv[...]
    for r in range(T):
        for s in range(2):
            for b in range(R):
                start = b * blk + r * q + s * h
                bsrc[r * 2 + s, 0:1, b * h : (b + 1) * h] = both[:, start : start + h]
    ball[t] = bsrc[...]
    valid = pair_valid[...].astype(F32)
    csrc[...] = jnp.broadcast_to(jnp.sum(valid, axis=1, keepdims=True), csrc.shape)

    for c in range(strips):
        own_copy(c).wait()
    pl.semaphore_wait(barrier, T - 1 + N - 1)

    def peer_copy(src, dst, send, recv, d):
        return pltpu.make_async_remote_copy(
            src_ref=src,
            dst_ref=dst.at[d],
            send_sem=send.at[d],
            recv_sem=recv.at[d],
            device_id=replica((me + d) % N),
            device_id_type=MESH,
        )

    def rank_copy(src, dst, send, recv, r):
        return pltpu.make_async_remote_copy(
            src_ref=src,
            dst_ref=dst,
            send_sem=send.at[r],
            recv_sem=recv.at[r],
            device_id=rank(flip(t, r, bits)),
            device_id_type=MESH,
        )

    def both_copy(r):
        return rank_copy(bsrc, ball.at[t], b_send, b_recv, r)

    def block_rows(outer, b):
        return outer * Z + b

    def ag_copy(b, c, send, where):
        return pltpu.make_async_remote_copy(
            src_ref=attn_all.at[block_rows(o, b), c],
            dst_ref=attn_all.at[block_rows(o, b), c],
            send_sem=send,
            recv_sem=ag_recv.at[o, b, c],
            device_id=where,
            device_id_type=MESH,
        )

    def right_copy(s, c):
        return ag_copy((p + Z - s) % Z, c, ag_right.at[s, c], (o, (p + 1) % Z, t))

    def left_copy(s, c):
        return ag_copy((p + s) % Z, c, ag_left.at[s, c], (o, (p + Z - 1) % Z, t))

    def right_sends(s):
        return (p >= s) & (p < Z - 1)

    def left_sends(s):
        return (p + s < Z) & (p > 0)

    def out_copy(b, e, c):
        return ag_copy(b, c, ag_out.at[e, b, c], ((o + e) % O, p, t))

    def arrived(outer, b, c):
        rows = attn_all.at[block_rows(outer, b), c]
        return pltpu.make_async_remote_copy(
            src_ref=rows,
            dst_ref=rows,
            send_sem=ag_out.at[0, 0, c],
            recv_sem=ag_recv.at[outer, b, c],
            device_id=(o, (p + 1) % Z, t),
            device_id_type=MESH,
        )

    def arrival(s, c):
        for ok, b in ((p - 1 - s >= 0, (p + Z - 1 - s) % Z), (p + 1 + s < Z, (p + 1 + s) % Z)):

            @pl.when(ok)
            def _():
                arrived(o, b, c).wait_recv()
                for e in range(1, O):
                    out_copy(b, e, c).start()

        if s + 1 < Z - 1:
            for ok, copy in ((right_sends(s + 1), right_copy), (left_sends(s + 1), left_copy)):

                @pl.when(ok)
                def _():
                    copy(s + 1, c).start()

    def arrivals(s):
        def one(c, carry):
            arrival(s, c)
            return carry

        lax.fori_loop(0, strips, one, 0)

    for ok, copy in ((right_sends(0), right_copy), (left_sends(0), left_copy)):

        @pl.when(ok)
        def _():
            for c in range(strips):
                copy(0, c).start()

    for r in range(1, T):
        both_copy(r).start()
    for d in range(1, N):
        peer_copy(csrc, cin, c_send, c_recv, d).start()
    for e in range(1, O):
        for c in range(strips):
            out_copy(p, e, c).start()

    def turn_attn(x, carry):
        rows = pl.ds(pl.multiple_of(x * 128, 128), 128)
        per = wide // 128
        cols = pl.ds(pl.multiple_of((x % per) * 128, 128), 128)
        attn_t[rows, :] = attn_all[me, x // per, :, cols].astype(F32).T.astype(BF16)
        return carry

    lax.fori_loop(0, attn.shape[1] // 128, turn_attn, 0)
    resid_copy.wait()

    def turn_resid(c, carry):
        cols = pl.ds(pl.multiple_of(c * 128, 128), 128)
        res_t[cols, :] = res_v[:, cols].astype(F32).T.astype(BF16)
        return carry

    lax.fori_loop(0, feats // 128, turn_resid, 0)
    hacc[...] = jnp.zeros_like(hacc)

    def rs_copy(s, j, g, mask):
        return pltpu.make_async_remote_copy(
            src_ref=part.at[s, j, g],
            dst_ref=got.at[s, j, g],
            send_sem=rs_send.at[s, j, g],
            recv_sem=rs_recv.at[s, j, g],
            device_id=rank(flip(t, mask, bits)),
            device_id_type=MESH,
        )

    def rs_mask(s, b):
        return s * 2**b + (1 - s) * 2 ** (bits - 1 - b)

    row16 = lax.broadcasted_iota(jnp.int32, (16, R * h), 0)

    def thirds(row):
        first = row.astype(BF16).astype(F32)
        second = (row - first).astype(BF16).astype(F32)
        third = row - first - second
        rows = jnp.where(row16 == 0, first, jnp.where(row16 == 1, second, third))
        return jnp.where(row16 < 3, rows, 0.0).astype(BF16)

    def add_heads(i):
        s, j, g = piece_of(i)
        r = target(s, j)
        total = hacc[...]
        for n in range(half):
            lhs = thirds(ball[g * half + n, r * 2 + s])
            rows = vbuf[i % 2, n * R * h : (n + 1) * R * h, :]
            high = rows.astype(BF16)
            low = (rows - high.astype(F32)).astype(BF16)
            total = total + jnp.dot(lhs, high, preferred_element_type=F32)
            total = total + jnp.dot(lhs, low, preferred_element_type=F32)
        hacc[...] = total

    def project(i, carry):
        @pl.when(i + SLOTS - 1 < steps)
        def _():
            load(i + SLOTS - 1).start()

        load(i).wait()
        s, j, g = piece_of(i)
        r = target(s, j)
        now = vbuf.at[i % 2]
        now[...] = jnp.dot(
            wbuf[i % SLOTS].reshape(K, wbuf.shape[3]), attn_t[...], preferred_element_type=F32
        )

        @pl.when(t // half == g)
        def _():
            for b in range(R):
                rows = pl.ds(pl.multiple_of(((t % half) * R + b) * h, h), h)
                mine = pl.ds(pl.multiple_of(b * blk + (r * 2 + s) * h, h), h)
                now[rows, :] = now[rows, :] + res_t[mine, :].astype(F32)

        @pl.when(j >= half)
        def _():
            part[s, j, g] = now[...].astype(BF16)
            rs_copy(s, j, g, rs_mask(s, bits - 1)).start()

        @pl.when(j < half)
        def _():
            keep[s, j % half, g] = now[...]

        @pl.when(i == 1)
        def _():
            for r in range(1, T):
                both_copy(r).wait_recv()

        @pl.when(i >= 1)
        def _():
            add_heads(i - 1)

        return carry

    lax.fori_loop(0, steps, project, 0)
    add_heads(steps - 1)

    for b in range(bits - 2, -1, -1):

        def combine(x, carry, b=b):
            j, s, g = 2**b + x // 4, x % 2, (x // 2) % 2
            total = keep[s, j, g]
            for up in range(b + 1, bits):
                rs_copy(s, j + 2**up, g, rs_mask(s, up)).wait_recv()
                total = total + got[s, j + 2**up, g].astype(F32)
            part[s, j, g] = total.astype(BF16)
            rs_copy(s, j, g, rs_mask(s, b)).start()
            return carry

        lax.fori_loop(0, 4 * 2**b, combine, 0)

    arrivals(0)

    def clear(j, carry):
        grad[pl.ds(pl.multiple_of(j * 128, 128), 128), :] = jnp.zeros((128, grad.shape[1]), F32)
        return carry

    lax.fori_loop(0, blk // 128, clear, 0)
    span = R * h
    diag = lax.broadcasted_iota(jnp.int32, (span, span), 0) == lax.broadcasted_iota(
        jnp.int32, (span, span), 1
    )

    def columns(x, carry):
        s, n = x % 2, x // 2
        row = jnp.broadcast_to(ball[n, t * 2 + s], (span, span))
        col = jnp.sum(jnp.where(diag, row, 0.0), axis=1, keepdims=True)
        rows = pl.ds(pl.multiple_of((n % half) * span, span), span)
        bcol[s, n // half, rows, :] = jnp.broadcast_to(col, (span, 128))
        return carry

    lax.fori_loop(0, 2 * T, columns, 0)

    S = lengths.shape[1]
    lens = lengths[...].astype(F32)
    same = lax.broadcasted_iota(jnp.int32, (S, S), 0) == lax.broadcasted_iota(jnp.int32, (S, S), 1)
    lens = jnp.sum(jnp.where(same, jnp.broadcast_to(lens, (S, S)), 0.0), axis=1, keepdims=True)
    seq_len = tok // S
    slot = lax.broadcasted_iota(jnp.int32, (S, tok), 1) - seq_len * lax.broadcasted_iota(
        jnp.int32, (S, tok), 0
    )
    live = (slot >= 0) & (slot.astype(F32) < lens)
    pool = jnp.where(live, 1.0 / lens, 0.0)
    who = lax.broadcasted_iota(jnp.int32, (S, pairs.shape[1]), 0)
    select = jnp.where(who == pairs[0:1, :], 1.0, 0.0) - jnp.where(who == pairs[1:2, :], 1.0, 0.0)

    def final(x, squares):
        s, g = x % 2, x // 2
        total = keep[s, 0, g]
        for up in range(bits - 1, -1, -1):
            rs_copy(s, 2**up, g, rs_mask(s, up)).wait_recv()
            total = total + got[s, 2**up, g].astype(F32)
        keep[s, 0, g] = total
        return squares + jnp.sum(total * total, axis=0, keepdims=True)

    squares = lax.fori_loop(0, 4, final, jnp.zeros((1, tok), F32))
    heads = jnp.sum(hacc[...], axis=0, keepdims=True)
    stat[0:1, :] = squares
    stat[1:2, :] = heads

    def stat_copy(r):
        return rank_copy(stat, stat_in.at[r], st_send, st_recv, r)

    for r in range(1, T):
        stat_copy(r).start()
    count = csrc[0:1, 0:1]
    for d in range(1, N):
        peer_copy(csrc, cin, c_send, c_recv, d).wait_recv()
        count = count + cin[d, 0:1, 0:1]
    for r in range(1, T):
        stat_copy(r).wait_recv()
        squares = squares + stat_in[r, 0:1, :]
        heads = heads + stat_in[r, 1:2, :]
    inv = 1.0 / jnp.sqrt(squares / width + 1e-05)
    score = heads * inv
    reward = jnp.sum(pool * score, axis=1, keepdims=True)
    margin = jnp.sum(select * reward, axis=0, keepdims=True)
    soft = jnp.maximum(-margin, 0.0) + jnp.log1p(jnp.exp(-jnp.abs(margin)))
    loss = jnp.sum(valid * soft, axis=1, keepdims=True)
    dmargin = -loss_scale[...] * valid * jax.nn.sigmoid(-margin) / count
    dreward = jnp.sum(select * dmargin, axis=1, keepdims=True)
    dscore = jnp.sum(pool * dreward, axis=0, keepdims=True)
    scale = inv * dscore
    pull = inv * inv * inv * dscore * heads / width

    def make_dproj(x, carry):
        s, g, n = x % 2, x // N, (x // 2) % (N // 2)
        rows = pl.ds(pl.multiple_of(n * h, h), h)
        spot = pl.ds(pl.multiple_of(s * h, h), h)
        for c in range(tok // 128):
            cols = slice(c * 128, (c + 1) * 128)
            dp[g * (N // 2) + n, spot, cols] = (
                scale[:, cols] * bcol[s, g, rows, :] - keep[s, 0, g, rows, cols] * pull[:, cols]
            ).astype(BF16)
        return carry

    lax.fori_loop(0, 2 * N, make_dproj, 0)

    side = p // (Z - Z // 2)
    edge = side * (Z - 1 - p) + (1 - side) * p

    def place(i):
        n = i // O
        past = (n + Z - 1 - edge) // Z
        spot = past * n + (1 - past) * (edge - n)
        return ((o + i) % O) * Z + side * (Z - 1 - spot) + (1 - side) * spot

    def slot_rows(r):
        return pl.ds(pl.multiple_of(r * q, q), q)

    def piece_copy(k):
        return pltpu.make_async_remote_copy(
            src_ref=dp.at[k],
            dst_ref=exch.at[me, slot_rows(t)],
            send_sem=z_send.at[k],
            recv_sem=z_recv.at[me],
            device_id=replica(k),
            device_id_type=MESH,
        )

    def piece_arrived(k):
        rows = exch.at[k, slot_rows(t)]
        return pltpu.make_async_remote_copy(
            src_ref=rows,
            dst_ref=rows,
            send_sem=z_send.at[k],
            recv_sem=z_recv.at[k],
            device_id=replica((me + 1) % N),
            device_id_type=MESH,
        )

    own_piece = pltpu.make_async_copy(dp.at[me], exch.at[me, slot_rows(t)], z_recv.at[me])
    own_piece.start()

    def send_piece(i, carry):
        piece_copy(place(i)).start()
        return carry

    lax.fori_loop(1, N, send_piece, 0)

    lsrc[...] = jnp.broadcast_to(loss, lsrc.shape)
    for s in range(2):
        for g in range(2):
            zw = keep[s, 0, g] * scale
            lanes = zw[:, 0:128]
            for c in range(1, tok // 128):
                lanes = lanes + zw[:, c * 128 : (c + 1) * 128]
            qsrc[s * 2 + g] = jnp.sum(lanes.T, axis=0, keepdims=True)
    for d in range(1, N):
        peer_copy(lsrc, lin, l_send, l_recv, d).start()
        peer_copy(qsrc, qin, q_send, q_recv, d).start()

    def ag_mask(s, b):
        return 2**b if s == 0 else 2 ** (bits - 1 - b)

    def held(s, c):
        return flip(t, c if s == 0 else reverse(c, bits), bits)

    def half_rows(r, s):
        return pl.ds(pl.multiple_of((r * 2 + s) * h, h), h)

    def spread_copy(k, s, c, b):
        rows = exch.at[k, half_rows(held(s, c), s)]
        return pltpu.make_async_remote_copy(
            src_ref=rows,
            dst_ref=rows,
            send_sem=e_send.at[k, s, c + 2**b],
            recv_sem=e_recv.at[k, s, c + 2**b],
            device_id=rank(flip(t, ag_mask(s, b), bits)),
            device_id_type=MESH,
        )

    def spread_arrived(k, s, c):
        rows = exch.at[k, half_rows(held(s, c), s)]
        return pltpu.make_async_remote_copy(
            src_ref=rows,
            dst_ref=rows,
            send_sem=e_send.at[k, s, c],
            recv_sem=e_recv.at[k, s, c],
            device_id=rank(flip(t, 1, bits)),
            device_id_type=MESH,
        )

    def begin(i):
        k = place(i)

        @pl.when(k == me)
        def _():
            own_piece.wait()

        @pl.when(k != me)
        def _():
            piece_arrived(k).wait_recv()

        for b in range(bits):
            for s in range(2):
                spread_copy(k, s, 0, b).start()

    def relay(i):
        k = place(i)
        for b in range(bits - 1):
            for c in range(2**b, 2 ** (b + 1)):
                for s in range(2):
                    spread_arrived(k, s, c).wait_recv()
                    for up in range(b + 1, bits):
                        spread_copy(k, s, c, up).start()

    def add_dot(k, c):
        grad[:, strip(c)] += jnp.dot(exch[k], attn_all[k, c], preferred_element_type=F32)

    def rows_ready(k):
        for c in range(half, T):
            for s in range(2):
                spread_arrived(k, s, c).wait_recv()

    def multiply(i):
        k = place(i)
        rows_ready(k)

        def one(c, carry):
            @pl.when(k // Z != o)
            def _():
                arrived(k // Z, k % Z, c).wait_recv()

            add_dot(k, c)
            return carry

        lax.fori_loop(0, strips, one, 0)

    def last_strips(c, carry):
        @pl.when(c < strips)
        def _():
            arrival(Z - 2, c)
            add_dot(place(N - O), c)

        @pl.when(c > 0)
        def _():
            for e in range(1, O):
                k = place(N - O + e)
                arrived(k // Z, k % Z, c - 1).wait_recv()
                add_dot(k, c - 1)

        return carry

    def gather_q():
        total = qsrc[...]
        for d in range(1, N):
            peer_copy(qsrc, qin, q_send, q_recv, d).wait_recv()
            total = total + qin[d]
        qsum[...] = total
        qall[t] = total
        for r in range(1, T):
            rank_copy(qsum, qall.at[t], t_send, t_recv, r).start()

    def finish_q():
        ltotal = lsrc[...]
        for d in range(1, N):
            peer_copy(lsrc, lin, l_send, l_recv, d).wait_recv()
            ltotal = ltotal + lin[d]
        loss_out[...] = ltotal[0:1, 0:1] / count
        for r in range(1, T):
            rank_copy(qsum, qall.at[t], t_send, t_recv, r).wait_recv()
        for r in range(T):
            for s in range(2):
                for b in range(R):
                    value = jnp.zeros((1, h), F32)
                    for owner in range(T):
                        n = (owner % half) * R + b
                        row = qall[r, s * 2 + owner // half]
                        value = jnp.where(t == owner, row[:, n * h : (n + 1) * h], value)
                    cols = slice(b * blk + r * q + s * h, b * blk + r * q + (s + 1) * h)
                    ggain[:, cols] = value * headv[:, cols]
                    ghead[:, cols] = value * gain[:, cols]

    def stage(i, carry):
        @pl.when(i < N)
        def _():
            begin(i)

        for s in range(1, Z - 2):

            @pl.when(i == (1 if s == 1 else 2 + (s + 1) * O))
            def _():
                arrivals(s)

        @pl.when(i >= 1)
        def _():
            relay(i - 1)

        @pl.when(i == N // 2 + 1)
        def _():
            gather_q()

        @pl.when(i == N)
        def _():
            finish_q()

        @pl.when((i >= 2) & (i < N + 2 - O))
        def _():
            multiply(i - 2)

        return carry

    lax.fori_loop(0, N + 1, stage, 0)
    for e in range(O):
        rows_ready(place(N - O + e))
    lax.fori_loop(0, strips + 1, last_strips, 0)

    for s in range(Z - 1):
        for ok, copy in ((right_sends(s), right_copy), (left_sends(s), left_copy)):

            @pl.when(ok)
            def _():
                for c in range(strips):
                    copy(s, c).wait_send()

    for e in range(1, O):
        for b in range(Z):
            for c in range(strips):
                out_copy(b, e, c).wait_send()
    for d in range(1, N):
        peer_copy(csrc, cin, c_send, c_recv, d).wait_send()
        peer_copy(lsrc, lin, l_send, l_recv, d).wait_send()
        peer_copy(qsrc, qin, q_send, q_recv, d).wait_send()
    for r in range(1, T):
        both_copy(r).wait_send()
        stat_copy(r).wait_send()
        rank_copy(qsum, qall.at[t], t_send, t_recv, r).wait_send()

    def rs_end(x, carry):
        s, g, j = x % 2, (x // 2) % 2, 1 + x // 4
        rs_copy(s, j, g, 1).wait_send()
        return carry

    lax.fori_loop(0, 4 * (T - 1), rs_end, 0)

    def send_end(i, carry):
        piece_copy(place(i)).wait_send()
        return carry

    lax.fori_loop(1, N, send_end, 0)

    def spread_end(k, carry):
        for b in range(bits):
            for c in range(2**b):
                for s in range(2):
                    spread_copy(k, s, c, b).wait_send()
        return carry

    lax.fori_loop(0, N, spread_end, 0)


def shards(sizes, attn, out_weight, resid, norm_gain, head, lengths, pairs, pair_valid, loss_scale):
    T, O, Z = sizes
    N = O * Z
    tok, feats = resid.shape
    width = feats * T
    blk = width // N
    q = blk // T
    h = q // 2
    K = (N // 2) * h
    R = N // T
    heads_dev = attn.shape[1]
    strips = heads_dev // min(512, heads_dev)
    vmem = pl.BlockSpec(memory_space=pltpu.VMEM)
    anyw = pl.BlockSpec(memory_space=pl.ANY)
    sem = pltpu.SemaphoreType.DMA
    bits = bits_of(T)
    grad_out_proj, grad_gain, grad_head, loss = pl.pallas_call(
        functools.partial(kernel, sizes),
        out_shape=(
            pltpu.VMEM((blk, heads_dev), F32),
            jax.ShapeDtypeStruct((1, feats), F32),
            jax.ShapeDtypeStruct((1, feats), F32),
            jax.ShapeDtypeStruct((1, 1), F32),
        ),
        in_specs=[anyw] * 3 + [vmem] * 6,
        out_specs=(vmem, vmem, vmem, vmem),
        scratch_shapes=[
            pltpu.VMEM((N, blk, tok), BF16),
            pltpu.VMEM((N, strips, tok, heads_dev // strips), BF16),
            pltpu.VMEM((SLOTS, N // 2, h, heads_dev), BF16),
            pltpu.VMEM((heads_dev, tok), BF16),
            pltpu.VMEM((tok, feats), BF16),
            pltpu.VMEM((feats, tok), BF16),
            pltpu.VMEM((1, feats), F32),
            pltpu.VMEM((1, feats), F32),
            pltpu.VMEM((2, K, tok), F32),
            pltpu.VMEM((2, T, 2, K, tok), BF16),
            pltpu.VMEM((2, T, 2, K, tok), BF16),
            pltpu.VMEM((2, T // 2, 2, K, tok), F32),
            pltpu.VMEM((N, q, tok), BF16),
            pltpu.VMEM((2 * T, 1, R * h), F32),
            pltpu.VMEM((T, 2 * T, 1, R * h), F32),
            pltpu.VMEM((2, 2, K, 128), F32),
            pltpu.VMEM((16, tok), F32),
            pltpu.VMEM((2, tok), F32),
            pltpu.VMEM((T, 2, tok), F32),
            pltpu.VMEM((8, 128), F32),
            pltpu.VMEM((N, 8, 128), F32),
            pltpu.VMEM((8, 128), F32),
            pltpu.VMEM((N, 8, 128), F32),
            pltpu.VMEM((4, 1, K), F32),
            pltpu.VMEM((N, 4, 1, K), F32),
            pltpu.VMEM((4, 1, K), F32),
            pltpu.VMEM((T, 4, 1, K), F32),
            sem((SLOTS,)),
            sem((2, T, 2)),
            sem((2, T, 2)),
            sem((T,)),
            sem((T,)),
            sem((T,)),
            sem((T,)),
            sem((N,)),
            sem((N,)),
            sem((N,)),
            sem((N,)),
            sem((N,)),
            sem((N,)),
            sem((T,)),
            sem((T,)),
            sem((strips,)),
            sem,
            sem((Z, strips)),
            sem((Z, strips)),
            sem((O, Z, strips)),
            sem((O, Z, strips)),
            sem((N,)),
            sem((N,)),
            sem((N, 2, T)),
            sem((N, 2, T)),
        ],
        compiler_params=pltpu.CompilerParams(
            collective_id=0, has_side_effects=True, vmem_limit_bytes=50 * 1024 * 1024
        ),
    )(
        attn,
        out_weight.reshape(N, 2 * T, h, heads_dev),
        resid,
        norm_gain.reshape(feats // 128, 128),
        head.reshape(feats // 128, 128),
        lengths[None, :],
        pairs.T,
        pair_valid[None, :],
        loss_scale[None, :],
    )
    return (loss.reshape(1), grad_out_proj, grad_gain[0], grad_head[0])


def solution(mesh):
    sizes = (mesh.shape["tensor"], mesh.shape["outer"], mesh.shape["dp"])
    return jax.shard_map(
        functools.partial(shards, sizes),
        mesh=mesh,
        in_specs=(
            P(("outer", "dp"), "tensor"),
            P(None, "tensor"),
            P(("outer", "dp"), "tensor"),
            P("tensor"),
            P("tensor"),
            P(("outer", "dp")),
            P(("outer", "dp"), None),
            P(("outer", "dp")),
            P(),
        ),
        out_specs=(P(), P(("outer", "dp"), "tensor"), P("tensor"), P("tensor")),
        check_vma=False,
    )
```

```python
import functools

import jax
import jax.numpy as jnp
from jax import lax
from jax.experimental import pallas as pl
from jax.experimental.pallas import tpu as pltpu
from jax.sharding import PartitionSpec as P

MESH = pl.DeviceIdType.MESH
F32 = jnp.float32
BF16 = jnp.bfloat16
SLOTS = 5
PARTS = 8


def bits_of(count):
    return count.bit_length() - 1


def flip(index, mask, bits):
    out = 0
    for j in range(bits):
        out = out + ((index // 2**j + mask // 2**j) % 2) * 2**j
    return out


def reverse(index, bits):
    out = 0
    for j in range(bits):
        out = out + ((index // 2**j) % 2) * 2 ** (bits - 1 - j)
    return out


def kernel(
    sizes,
    attn,
    weight,
    resid,
    gain_in,
    head_in,
    lengths,
    pairs,
    pair_valid,
    loss_scale,
    grad,
    ggain,
    ghead,
    loss_out,
    exch,
    attn_all,
    wbuf,
    attn_t,
    res_v,
    res_t,
    gain,
    headv,
    vbuf,
    part,
    got,
    keep,
    dp,
    bsrc,
    ball,
    bcol,
    hacc,
    stat,
    stat_in,
    csrc,
    cin,
    lsrc,
    lin,
    qsrc,
    qin,
    qsum,
    qall,
    wsem,
    rs_send,
    rs_recv,
    b_send,
    b_recv,
    st_send,
    st_recv,
    c_send,
    c_recv,
    l_send,
    l_recv,
    q_send,
    q_recv,
    t_send,
    t_recv,
    ag_local,
    r_local,
    ag_right,
    ag_left,
    ag_out,
    ag_recv,
    z_send,
    z_recv,
    e_send,
    e_recv,
):
    T, O, Z = sizes
    N = O * Z
    bits = bits_of(T)
    R = N // T
    half = T // 2
    tok, feats = resid.shape
    width = feats * T
    blk = width // N
    q = blk // T
    h = q // 2
    K = (N // 2) * h
    steps = 4 * T
    strips, wide = attn_all.shape[1], attn_all.shape[3]
    o, p, t = lax.axis_index("outer"), lax.axis_index("dp"), lax.axis_index("tensor")
    me = o * Z + p

    def replica(k):
        return (k // Z, k % Z, t)

    def rank(r):
        return (o, p, r)

    barrier = pltpu.get_barrier_semaphore()
    for r in range(1, T):
        pl.semaphore_signal(barrier, inc=1, device_id=rank(flip(t, r, bits)), device_id_type=MESH)
    for d in range(1, N):
        pl.semaphore_signal(barrier, inc=1, device_id=replica((me + d) % N), device_id_type=MESH)

    def piece_of(i):
        e, g = i // 2, i % 2
        s = e % 2
        j = T - 1 - e // 2
        return s, j, g

    def target(s, j):
        return flip(t, s * j + (1 - s) * reverse(j, bits), bits)

    def load(i):
        s, j, g = piece_of(i)
        return pltpu.make_async_copy(
            weight.at[pl.ds(g * (N // 2), N // 2), target(s, j) * 2 + s],
            wbuf.at[i % SLOTS],
            wsem.at[i % SLOTS],
        )

    def strip(c):
        return pl.ds(pl.multiple_of(c * wide, wide), wide)

    def own_copy(c):
        return pltpu.make_async_copy(attn.at[:, strip(c)], attn_all.at[me, c], ag_local.at[c])

    resid_copy = pltpu.make_async_copy(resid, res_v, r_local)
    for c in range(strips):
        own_copy(c).start()
    load(0).start()
    resid_copy.start()
    pl.semaphore_wait(barrier, T - 1 + N - 1)

    def peer_copy(src, dst, send, recv, d):
        return pltpu.make_async_remote_copy(
            src_ref=src,
            dst_ref=dst.at[d],
            send_sem=send,
            recv_sem=recv,
            device_id=replica((me + d) % N),
            device_id_type=MESH,
        )

    def rank_copy(src, dst, send, recv, r):
        return pltpu.make_async_remote_copy(
            src_ref=src,
            dst_ref=dst,
            send_sem=send,
            recv_sem=recv,
            device_id=rank(flip(t, r, bits)),
            device_id_type=MESH,
        )

    def wait_all(ref, sem):
        pltpu.make_async_copy(ref, ref, sem).wait()

    def both_copy(r):
        return rank_copy(bsrc, ball.at[t], b_send, b_recv, r)

    def block_rows(outer, b):
        return outer * Z + b

    def ag_copy(b, c, send, where, own=False):
        return pltpu.make_async_remote_copy(
            src_ref=attn.at[:, strip(c)] if own else attn_all.at[block_rows(o, b), c],
            dst_ref=attn_all.at[block_rows(o, b), c],
            send_sem=send,
            recv_sem=ag_recv.at[o, b, c],
            device_id=where,
            device_id_type=MESH,
        )

    def right_copy(s, c):
        return ag_copy((p + Z - s) % Z, c, ag_right.at[s], (o, (p + 1) % Z, t), s == 0)

    def left_copy(s, c):
        return ag_copy((p + s) % Z, c, ag_left.at[s], (o, (p + Z - 1) % Z, t), s == 0)

    def right_sends(s):
        return (p >= s) & (p < Z - 1)

    def left_sends(s):
        return (p + s < Z) & (p > 0)

    def out_copy(b, e, c):
        return ag_copy(b, c, ag_out.at[e], ((o + e) % O, p, t))

    def arrived(outer, b, c):
        rows = attn_all.at[block_rows(outer, b), c]
        return pltpu.make_async_remote_copy(
            src_ref=rows,
            dst_ref=rows,
            send_sem=ag_out.at[0],
            recv_sem=ag_recv.at[outer, b, c],
            device_id=(o, (p + 1) % Z, t),
            device_id_type=MESH,
        )

    def arrival(s, c, ends=False):
        for ok, b in ((p - 1 - s >= 0, (p + Z - 1 - s) % Z), (p + 1 + s < Z, (p + 1 + s) % Z)):

            @pl.when(ok)
            def _():
                arrived(o, b, c).wait_recv()
                for e in range(1, O):
                    out_copy(b, e, c).start()

        if s + 1 < Z - 1:
            for ok, copy in relays(s + 1, ends):

                @pl.when(ok)
                def _():
                    copy(s + 1, c).start()

    def relays(s, ends=False, inner=False):
        right, left = right_sends(s), left_sends(s)
        if ends:
            right, left = right & (p + 2 == Z), left & (p == 1)
        if inner:
            right, left = right & (p + 2 < Z), left & (p > 1)
        return (right, right_copy), (left, left_copy)

    def arrivals(s, first, last, ends=False):
        def one(c, carry):
            arrival(s, c, ends)
            return carry

        lax.fori_loop(first, last, one, 0)

    for ok, copy in ((right_sends(0), right_copy), (left_sends(0), left_copy)):

        @pl.when(ok)
        def _():
            for c in range(strips):
                copy(0, c).start()

    lanes = gain_in.shape[1]
    for c in range(feats // lanes):
        gain[:, c * lanes : (c + 1) * lanes] = gain_in[c : c + 1, :].astype(F32)
        headv[:, c * lanes : (c + 1) * lanes] = head_in[c : c + 1, :].astype(F32)
    both = gain[...] * headv[...]
    for r in range(T):
        for s in range(2):
            for b in range(R):
                start = b * blk + r * q + s * h
                bsrc[r * 2 + s, 0:1, b * h : (b + 1) * h] = both[:, start : start + h]
    ball[t] = bsrc[...]
    valid = pair_valid[...].astype(F32)
    csrc[...] = jnp.broadcast_to(jnp.sum(valid, axis=1, keepdims=True), csrc.shape)

    for r in range(1, T):
        both_copy(r).start()
    for d in range(1, N):
        peer_copy(csrc, cin, c_send, c_recv, d).start()
    for c in range(strips):
        own_copy(c).wait()
        for e in range(1, O):
            out_copy(p, e, c).start()
    for i in range(1, min(SLOTS - 1, steps)):
        load(i).start()

    def turn_attn(x, carry):
        rows = pl.ds(pl.multiple_of(x * 128, 128), 128)
        per = wide // 128
        cols = pl.ds(pl.multiple_of((x % per) * 128, 128), 128)
        attn_t[rows, :] = attn_all[me, x // per, :, cols].T
        return carry

    lax.fori_loop(0, attn.shape[1] // 128, turn_attn, 0)
    resid_copy.wait()

    if h % 128 > 0:

        def turn_resid(c, carry):
            cols = pl.ds(pl.multiple_of(c * 128, 128), 128)
            res_t[cols, :] = res_v[:, cols].T
            return carry

        lax.fori_loop(0, feats // 128, turn_resid, 0)

    hacc[...] = jnp.zeros_like(hacc)

    def rs_copy(s, j, g, mask):
        return pltpu.make_async_remote_copy(
            src_ref=part.at[s, j, g],
            dst_ref=got.at[s, j, g],
            send_sem=rs_send,
            recv_sem=rs_recv.at[s, j - 1, g],
            device_id=rank(flip(t, mask, bits)),
            device_id_type=MESH,
        )

    def rs_mask(s, b):
        return s * 2**b + (1 - s) * 2 ** (bits - 1 - b)

    row16 = lax.broadcasted_iota(jnp.int32, (16, R * h), 0)

    def thirds(row):
        first = row.astype(BF16).astype(F32)
        second = (row - first).astype(BF16).astype(F32)
        third = row - first - second
        rows = jnp.where(row16 == 0, first, jnp.where(row16 == 1, second, third))
        return jnp.where(row16 < 3, rows, 0.0).astype(BF16)

    def add_heads(i):
        s, j, g = piece_of(i)
        r = target(s, j)
        total = hacc[...]
        for n in range(half):
            lhs = thirds(ball[g * half + n, r * 2 + s])
            rows = vbuf[i % 2, n * R * h : (n + 1) * R * h, :]
            high = rows.astype(BF16)
            low = (rows - high.astype(F32)).astype(BF16)
            total = total + jnp.dot(lhs, high, preferred_element_type=F32)
            total = total + jnp.dot(lhs, low, preferred_element_type=F32)
        hacc[...] = total

    def project(i, carry):
        @pl.when(i + SLOTS - 1 < steps)
        def _():
            load(i + SLOTS - 1).start()

        load(i).wait()
        s, j, g = piece_of(i)
        r = target(s, j)
        now = vbuf.at[i % 2]
        now[...] = jnp.dot(
            wbuf[i % SLOTS].reshape(K, wbuf.shape[3]), attn_t[...], preferred_element_type=F32
        )

        @pl.when(t // half == g)
        def _():
            for b in range(R):
                rows = pl.ds(pl.multiple_of(((t % half) * R + b) * h, h), h)
                mine = pl.ds(pl.multiple_of(b * blk + (r * 2 + s) * h, h), h)
                if h % 128 > 0:
                    extra = res_t[mine, :].astype(F32)
                else:
                    extra = res_v[:, mine].astype(F32).T
                now[rows, :] = now[rows, :] + extra

        @pl.when(j >= half)
        def _():
            part[s, j, g] = now[...].astype(BF16)
            rs_copy(s, j, g, rs_mask(s, bits - 1)).start()

        @pl.when(j < half)
        def _():
            keep[s, j % half, g] = now[...]

        @pl.when(i == 1)
        def _():
            wait_all(ball.at[pl.ds(0, T - 1)], b_recv)

        @pl.when(i >= 1)
        def _():
            add_heads(i - 1)

        return carry

    lax.fori_loop(0, steps, project, 0)
    add_heads(steps - 1)

    for b in range(bits - 2, -1, -1):

        def combine(x, carry, b=b):
            j, s, g = 2**b + x // 4, x % 2, (x // 2) % 2
            total = keep[s, j, g]
            for up in range(b + 1, bits):
                rs_copy(s, j + 2**up, g, rs_mask(s, up)).wait_recv()
                total = total + got[s, j + 2**up, g].astype(F32)
            part[s, j, g] = total.astype(BF16)
            rs_copy(s, j, g, rs_mask(s, b)).start()
            return carry

        lax.fori_loop(0, 4 * 2**b, combine, 0)

    early = max(1, strips - 1)
    arrivals(0, 0, early)
    arrivals(0, early, strips, True)

    def clear(j, carry):
        grad[pl.ds(pl.multiple_of(j * 128, 128), 128), :] = jnp.zeros((128, grad.shape[1]), F32)
        return carry

    lax.fori_loop(0, blk // 128, clear, 0)
    span = R * h
    diag = lax.broadcasted_iota(jnp.int32, (span, span), 0) == lax.broadcasted_iota(
        jnp.int32, (span, span), 1
    )

    def columns(x, carry):
        s, n = x % 2, x // 2
        row = jnp.broadcast_to(ball[n, t * 2 + s], (span, span))
        col = jnp.sum(jnp.where(diag, row, 0.0), axis=1, keepdims=True)
        rows = pl.ds(pl.multiple_of((n % half) * span, span), span)
        bcol[s, n // half, rows, :] = jnp.broadcast_to(col, (span, 128))
        return carry

    lax.fori_loop(0, 2 * T, columns, 0)

    S = lengths.shape[1]
    lens = lengths[...].astype(F32)
    same = lax.broadcasted_iota(jnp.int32, (S, S), 0) == lax.broadcasted_iota(jnp.int32, (S, S), 1)
    lens = jnp.sum(jnp.where(same, jnp.broadcast_to(lens, (S, S)), 0.0), axis=1, keepdims=True)
    seq_len = tok // S
    slot = lax.broadcasted_iota(jnp.int32, (S, tok), 1) - seq_len * lax.broadcasted_iota(
        jnp.int32, (S, tok), 0
    )
    live = (slot >= 0) & (slot.astype(F32) < lens)
    pool = jnp.where(live, 1.0 / lens, 0.0)
    who = lax.broadcasted_iota(jnp.int32, (S, pairs.shape[1]), 0)
    select = jnp.where(who == pairs[0:1, :], 1.0, 0.0) - jnp.where(who == pairs[1:2, :], 1.0, 0.0)

    def final(x, squares):
        s, g = x % 2, x // 2
        total = keep[s, 0, g]
        for up in range(bits - 1, -1, -1):
            rs_copy(s, 2**up, g, rs_mask(s, up)).wait_recv()
            total = total + got[s, 2**up, g].astype(F32)
        keep[s, 0, g] = total
        return squares + jnp.sum(total * total, axis=0, keepdims=True)

    squares = lax.fori_loop(0, 4, final, jnp.zeros((1, tok), F32))
    heads = jnp.sum(hacc[...], axis=0, keepdims=True)
    stat[0:1, :] = squares
    stat[1:2, :] = heads

    def stat_copy(r):
        return rank_copy(stat, stat_in.at[r], st_send, st_recv, r)

    for r in range(1, T):
        stat_copy(r).start()
    count = csrc[0:1, 0:1]
    wait_all(cin.at[pl.ds(1, N - 1)], c_recv)
    for d in range(1, N):
        count = count + cin[d, 0:1, 0:1]
    wait_all(stat_in.at[pl.ds(1, T - 1)], st_recv)
    for r in range(1, T):
        squares = squares + stat_in[r, 0:1, :]
        heads = heads + stat_in[r, 1:2, :]
    inv = 1.0 / jnp.sqrt(squares / width + 1e-05)
    score = heads * inv
    reward = jnp.sum(pool * score, axis=1, keepdims=True)
    margin = jnp.sum(select * reward, axis=0, keepdims=True)
    soft = jnp.maximum(-margin, 0.0) + jnp.log1p(jnp.exp(-jnp.abs(margin)))
    loss = jnp.sum(valid * soft, axis=1, keepdims=True)
    dmargin = -loss_scale[...] * valid * jax.nn.sigmoid(-margin) / count
    dreward = jnp.sum(select * dmargin, axis=1, keepdims=True)
    dscore = jnp.sum(pool * dreward, axis=0, keepdims=True)
    scale = inv * dscore
    pull = inv * inv * inv * dscore * heads / width

    def make_dproj(x, carry):
        s, g, n = x % 2, x // N, (x // 2) % (N // 2)
        rows = pl.ds(pl.multiple_of(n * h, h), h)
        spot = pl.ds(pl.multiple_of(s * h, h), h)
        for c in range(tok // 128):
            cols = slice(c * 128, (c + 1) * 128)
            dp[g * (N // 2) + n, spot, cols] = (
                scale[:, cols] * bcol[s, g, rows, :] - keep[s, 0, g, rows, cols] * pull[:, cols]
            ).astype(BF16)
        return carry

    lax.fori_loop(0, 2 * N, make_dproj, 0)

    side = p // (Z - Z // 2)
    edge = side * (Z - 1 - p) + (1 - side) * p

    def place(i):
        n = i // O
        past = (n + Z - 1 - edge) // Z
        spot = past * n + (1 - past) * (edge - n)
        return ((o + i) % O) * Z + side * (Z - 1 - spot) + (1 - side) * spot

    def slot_rows(r):
        return pl.ds(pl.multiple_of(r * q, q), q)

    def piece_copy(k):
        return pltpu.make_async_remote_copy(
            src_ref=dp.at[k],
            dst_ref=exch.at[me, slot_rows(t)],
            send_sem=z_send,
            recv_sem=z_recv.at[me],
            device_id=replica(k),
            device_id_type=MESH,
        )

    def piece_arrived(k):
        rows = exch.at[k, slot_rows(t)]
        return pltpu.make_async_remote_copy(
            src_ref=rows,
            dst_ref=rows,
            send_sem=z_send,
            recv_sem=z_recv.at[k],
            device_id=replica((me + 1) % N),
            device_id_type=MESH,
        )

    own_piece = pltpu.make_async_copy(dp.at[me], exch.at[me, slot_rows(t)], z_recv.at[me])
    own_piece.start()

    def send_piece(i, carry):
        piece_copy(place(i)).start()
        return carry

    lax.fori_loop(1, N // 2, send_piece, 0)

    @pl.when(edge > 0)
    def _():
        lax.fori_loop(N // 2, N, send_piece, 0)


    lsrc[...] = jnp.broadcast_to(loss, lsrc.shape)
    for s in range(2):
        for g in range(2):
            zw = keep[s, 0, g] * scale
            lanes = zw[:, 0:128]
            for c in range(1, tok // 128):
                lanes = lanes + zw[:, c * 128 : (c + 1) * 128]
            qsrc[s * 2 + g] = jnp.sum(lanes.T, axis=0, keepdims=True)
    for d in range(1, N):
        peer_copy(lsrc, lin, l_send, l_recv, d).start()
        peer_copy(qsrc, qin, q_send, q_recv, d).start()
    for c in range(early, strips):
        for ok, copy in relays(1, inner=True):

            @pl.when(ok)
            def _():
                copy(1, c).start()


    def ag_mask(s, b):
        return 2**b if s == 0 else 2 ** (bits - 1 - b)

    def held(s, c):
        return flip(t, c if s == 0 else reverse(c, bits), bits)

    def half_rows(r, s):
        return pl.ds(pl.multiple_of((r * 2 + s) * h, h), h)

    def spread_copy(k, s, c, b):
        rows = exch.at[k, half_rows(held(s, c), s)]
        return pltpu.make_async_remote_copy(
            src_ref=rows,
            dst_ref=rows,
            send_sem=e_send,
            recv_sem=e_recv.at[k, b],
            device_id=rank(flip(t, ag_mask(s, b), bits)),
            device_id_type=MESH,
        )

    def spread_arrived(k, b):
        wait_all(exch.at[k, pl.ds(0, q * 2**b)], e_recv.at[k, b])

    def begin(i):
        k = place(i)

        @pl.when(k == me)
        def _():
            own_piece.wait()

        @pl.when(k != me)
        def _():
            piece_arrived(k).wait_recv()

        for b in range(bits):
            for s in range(2):
                spread_copy(k, s, 0, b).start()

    def relay(i):
        k = place(i)
        for b in range(bits - 1):
            spread_arrived(k, b)
            for c in range(2**b, 2 ** (b + 1)):
                for s in range(2):
                    for up in range(b + 1, bits):
                        spread_copy(k, s, c, up).start()

    def add_dot(k, c):
        grad[:, strip(c)] += jnp.dot(exch[k], attn_all[k, c], preferred_element_type=F32)

    def rows_ready(k):
        spread_arrived(k, bits - 1)

    def multiply(i):
        k = place(i)
        rows_ready(k)

        def one(c, carry):
            @pl.when(k // Z != o)
            def _():
                arrived(k // Z, k % Z, c).wait_recv()

            add_dot(k, c)
            return carry

        lax.fori_loop(0, strips, one, 0)

    def last_strips(c, carry):
        @pl.when(c < strips)
        def _():
            arrival(Z - 2, c)
            add_dot(place(N - O), c)

        @pl.when(c > 0)
        def _():
            for e in range(1, O):
                k = place(N - O + e)
                arrived(k // Z, k % Z, c - 1).wait_recv()
                add_dot(k, c - 1)

        return carry

    def gather_q():
        total = qsrc[...]
        wait_all(qin.at[pl.ds(1, N - 1)], q_recv)
        for d in range(1, N):
            total = total + qin[d]
        qsum[...] = total
        qall[t] = total
        for r in range(1, T):
            rank_copy(qsum, qall.at[t], t_send, t_recv, r).start()

    def finish_q():
        ltotal = lsrc[...]
        wait_all(lin.at[pl.ds(1, N - 1)], l_recv)
        for d in range(1, N):
            ltotal = ltotal + lin[d]
        loss_out[...] = ltotal[0:1, 0:1] / count
        wait_all(qall.at[pl.ds(0, T - 1)], t_recv)
        for r in range(T):
            for s in range(2):
                for b in range(R):
                    value = jnp.zeros((1, h), F32)
                    for owner in range(T):
                        n = (owner % half) * R + b
                        row = qall[r, s * 2 + owner // half]
                        value = jnp.where(t == owner, row[:, n * h : (n + 1) * h], value)
                    cols = slice(b * blk + r * q + s * h, b * blk + r * q + (s + 1) * h)
                    ggain[:, cols] = value * headv[:, cols]
                    ghead[:, cols] = value * gain[:, cols]

    def stage(i, carry):
        @pl.when(i < N)
        def _():
            begin(i)

        @pl.when((i == O) & (edge == 0))
        def _():
            lax.fori_loop(N // 2, N, send_piece, 0)

        for s in range(1, Z - 2):

            @pl.when(i == (O if s == 1 else 2 + (s + 1) * O))
            def _():
                arrivals(s, 0, early if s == 1 else strips)

            if s == 1:

                @pl.when(i == 2 + 2 * O)
                def _():
                    arrivals(1, early, strips)

        @pl.when(i >= 1)
        def _():
            relay(i - 1)

        @pl.when(i == N - 2)
        def _():
            gather_q()

        @pl.when(i == N)
        def _():
            finish_q()

        @pl.when((i >= 2) & (i < N + 2 - O))
        def _():
            multiply(i - 2)

        return carry

    lax.fori_loop(0, N + 1, stage, 0)
    for e in range(O):
        rows_ready(place(N - O + e))
    lax.fori_loop(0, strips + 1, last_strips, 0)

    for s in range(Z - 1):
        for ok, sem in ((right_sends(s), ag_right), (left_sends(s), ag_left)):

            @pl.when(ok)
            def _():
                wait_all(attn_all.at[0], sem.at[s])

    for e in range(1, O):
        wait_all(attn_all.at[pl.ds(0, Z)], ag_out.at[e])
    wait_all(cin.at[pl.ds(1, N - 1)], c_send)
    wait_all(lin.at[pl.ds(1, N - 1)], l_send)
    wait_all(qin.at[pl.ds(1, N - 1)], q_send)
    wait_all(ball.at[pl.ds(0, T - 1)], b_send)
    wait_all(stat_in.at[pl.ds(1, T - 1)], st_send)
    wait_all(qall.at[pl.ds(0, T - 1)], t_send)
    wait_all(part.at[:, pl.ds(1, T - 1)], rs_send)
    wait_all(dp.at[pl.ds(0, N - 1)], z_send)
    wait_all(exch.at[:, pl.ds(0, (T - 1) * q)], e_send)


def write_out(grad, ggain, ghead, loss, grad_o, ggain_o, ghead_o, loss_o, sems):
    rows = grad.shape[0] // PARTS
    copies = []
    for i in range(PARTS):
        part = pl.ds(i * rows, rows)
        copies.append(pltpu.make_async_copy(grad.at[part], grad_o.at[part], sems.at[i]))
    for i, (src, dst) in enumerate(((ggain, ggain_o), (ghead, ghead_o), (loss, loss_o))):
        copies.append(pltpu.make_async_copy(src, dst, sems.at[PARTS + i]))
    for copy in copies:
        copy.start()
    for copy in copies:
        copy.wait()


def shards(sizes, attn, out_weight, resid, norm_gain, head, lengths, pairs, pair_valid, loss_scale):
    T, O, Z = sizes
    N = O * Z
    tok, feats = resid.shape
    width = feats * T
    blk = width // N
    q = blk // T
    h = q // 2
    K = (N // 2) * h
    R = N // T
    heads_dev = attn.shape[1]
    strips = heads_dev // min(512, heads_dev)
    vmem = pl.BlockSpec(memory_space=pltpu.VMEM)
    anyw = pl.BlockSpec(memory_space=pl.ANY)
    sem = pltpu.SemaphoreType.DMA
    bits = bits_of(T)
    results = pl.pallas_call(
        functools.partial(kernel, sizes),
        out_shape=(
            pltpu.VMEM((blk, heads_dev), F32),
            pltpu.VMEM((1, feats), F32),
            pltpu.VMEM((1, feats), F32),
            pltpu.VMEM((1, 1), F32),
        ),
        in_specs=[anyw] * 3 + [vmem] * 6,
        out_specs=(vmem, vmem, vmem, vmem),
        scratch_shapes=[
            pltpu.VMEM((N, blk, tok), BF16),
            pltpu.VMEM((N, strips, tok, heads_dev // strips), BF16),
            pltpu.VMEM((SLOTS, N // 2, h, heads_dev), BF16),
            pltpu.VMEM((heads_dev, tok), BF16),
            pltpu.VMEM((tok, feats), BF16),
            pltpu.VMEM((feats, tok), BF16),
            pltpu.VMEM((1, feats), F32),
            pltpu.VMEM((1, feats), F32),
            pltpu.VMEM((2, K, tok), F32),
            pltpu.VMEM((2, T, 2, K, tok), BF16),
            pltpu.VMEM((2, T, 2, K, tok), BF16),
            pltpu.VMEM((2, T // 2, 2, K, tok), F32),
            pltpu.VMEM((N, q, tok), BF16),
            pltpu.VMEM((2 * T, 1, R * h), F32),
            pltpu.VMEM((T, 2 * T, 1, R * h), F32),
            pltpu.VMEM((2, 2, K, 128), F32),
            pltpu.VMEM((16, tok), F32),
            pltpu.VMEM((2, tok), F32),
            pltpu.VMEM((T, 2, tok), F32),
            pltpu.VMEM((8, 128), F32),
            pltpu.VMEM((N, 8, 128), F32),
            pltpu.VMEM((8, 128), F32),
            pltpu.VMEM((N, 8, 128), F32),
            pltpu.VMEM((4, 1, K), F32),
            pltpu.VMEM((N, 4, 1, K), F32),
            pltpu.VMEM((4, 1, K), F32),
            pltpu.VMEM((T, 4, 1, K), F32),
            sem((SLOTS,)),
            sem,
            sem((2, T - 1, 2)),
            sem,
            sem,
            sem,
            sem,
            sem,
            sem,
            sem,
            sem,
            sem,
            sem,
            sem,
            sem,
            sem((strips,)),
            sem,
            sem((Z,)),
            sem((Z,)),
            sem((O,)),
            sem((O, Z, strips)),
            sem,
            sem((N,)),
            sem,
            sem((N, bits)),
        ],
        compiler_params=pltpu.CompilerParams(
            collective_id=0, has_side_effects=True, vmem_limit_bytes=50 * 1024 * 1024
        ),
    )(
        attn,
        out_weight.reshape(N, 2 * T, h, heads_dev),
        resid,
        norm_gain.reshape(feats // 128, 128),
        head.reshape(feats // 128, 128),
        lengths[None, :],
        pairs.T,
        pair_valid[None, :],
        loss_scale[None, :],
    )
    grad_out_proj, grad_gain, grad_head, loss = pl.pallas_call(
        write_out,
        out_shape=(
            jax.ShapeDtypeStruct((blk, heads_dev), F32),
            jax.ShapeDtypeStruct((1, feats), F32),
            jax.ShapeDtypeStruct((1, feats), F32),
            jax.ShapeDtypeStruct((1, 1), F32),
        ),
        in_specs=[anyw] * 4,
        out_specs=(anyw,) * 4,
        scratch_shapes=[sem((PARTS + 3,))],
        compiler_params=pltpu.CompilerParams(vmem_limit_bytes=1024 * 1024),
    )(*results)
    return (loss.reshape(1), grad_out_proj, grad_gain[0], grad_head[0])


def solution(mesh):
    sizes = (mesh.shape["tensor"], mesh.shape["outer"], mesh.shape["dp"])
    return jax.shard_map(
        functools.partial(shards, sizes),
        mesh=mesh,
        in_specs=(
            P(("outer", "dp"), "tensor"),
            P(None, "tensor"),
            P(("outer", "dp"), "tensor"),
            P("tensor"),
            P("tensor"),
            P(("outer", "dp")),
            P(("outer", "dp"), None),
            P(("outer", "dp")),
            P(),
        ),
        out_specs=(P(), P(("outer", "dp"), "tensor"), P("tensor"), P("tensor")),
        check_vma=False,
    )
```

```python
import functools

import jax
import jax.numpy as jnp
from jax import lax
from jax.experimental import pallas as pl
from jax.experimental.pallas import tpu as pltpu
from jax.sharding import PartitionSpec as P

MESH = pl.DeviceIdType.MESH
F32 = jnp.float32
BF16 = jnp.bfloat16
SLOTS = 5
PARTS = 8


def bits_of(count):
    return count.bit_length() - 1


def flip(index, mask, bits):
    out = 0
    for j in range(bits):
        out = out + ((index // 2**j + mask // 2**j) % 2) * 2**j
    return out


def reverse(index, bits):
    out = 0
    for j in range(bits):
        out = out + ((index // 2**j) % 2) * 2 ** (bits - 1 - j)
    return out


def encode(value):
    square = value * value
    return (value * jnp.abs(value) * square * (square * square)).astype(BF16)


def decode(code):
    code = code.astype(F32)
    size = jnp.sqrt(jnp.sqrt(jnp.sqrt(jnp.abs(code))))
    return jnp.where(code < 0.0, -size, size)


def kernel(
    sizes,
    attn,
    weight,
    resid,
    gain_in,
    head_in,
    lengths,
    pairs,
    pair_valid,
    loss_scale,
    grad,
    ggain,
    ghead,
    loss_out,
    exch,
    attn_all,
    wbuf,
    attn_t,
    res_v,
    res_t,
    gain,
    headv,
    vbuf,
    part,
    got,
    keep,
    dp,
    bsrc,
    ball,
    bcol,
    hacc,
    stat,
    stat_in,
    csrc,
    cin,
    lsrc,
    lin,
    qsrc,
    qin,
    qsum,
    qall,
    wsem,
    rs_send,
    rs_recv,
    b_send,
    b_recv,
    st_send,
    st_recv,
    c_send,
    c_recv,
    l_send,
    l_recv,
    q_send,
    q_recv,
    t_send,
    t_recv,
    ag_local,
    r_local,
    ag_right,
    ag_left,
    ag_out,
    ag_recv,
    z_send,
    z_recv,
    e_send,
    e_recv,
):
    T, O, Z = sizes
    N = O * Z
    bits = bits_of(T)
    R = N // T
    half = T // 2
    tok, feats = resid.shape
    width = feats * T
    blk = width // N
    q = blk // T
    h = q // 2
    K = (N // 2) * h
    steps = 4 * T
    strips, wide = attn_all.shape[1], attn_all.shape[3]
    o, p, t = lax.axis_index("outer"), lax.axis_index("dp"), lax.axis_index("tensor")
    me = o * Z + p

    def replica(k):
        return (k // Z, k % Z, t)

    def rank(r):
        return (o, p, r)

    barrier = pltpu.get_barrier_semaphore()
    for r in range(1, T):
        pl.semaphore_signal(barrier, inc=1, device_id=rank(flip(t, r, bits)), device_id_type=MESH)
    for d in range(1, N):
        pl.semaphore_signal(barrier, inc=1, device_id=replica((me + d) % N), device_id_type=MESH)

    def piece_of(i):
        e, g = i // 2, i % 2
        s = e % 2
        j = T - 1 - e // 2
        return s, j, g

    def target(s, j):
        return flip(t, s * j + (1 - s) * reverse(j, bits), bits)

    def load(i):
        s, j, g = piece_of(i)
        return pltpu.make_async_copy(
            weight.at[pl.ds(g * (N // 2), N // 2), target(s, j) * 2 + s],
            wbuf.at[i % SLOTS],
            wsem.at[i % SLOTS],
        )

    def strip(c):
        return pl.ds(pl.multiple_of(c * wide, wide), wide)

    def own_copy(c):
        return pltpu.make_async_copy(attn.at[:, strip(c)], attn_all.at[me, c], ag_local.at[c])

    resid_copy = pltpu.make_async_copy(resid, res_v, r_local)
    for c in range(strips):
        own_copy(c).start()
    load(0).start()
    resid_copy.start()
    pl.semaphore_wait(barrier, T - 1 + N - 1)

    def peer_copy(src, dst, send, recv, d):
        return pltpu.make_async_remote_copy(
            src_ref=src,
            dst_ref=dst.at[d],
            send_sem=send,
            recv_sem=recv,
            device_id=replica((me + d) % N),
            device_id_type=MESH,
        )

    def rank_copy(src, dst, send, recv, r):
        return pltpu.make_async_remote_copy(
            src_ref=src,
            dst_ref=dst,
            send_sem=send,
            recv_sem=recv,
            device_id=rank(flip(t, r, bits)),
            device_id_type=MESH,
        )

    def wait_all(ref, sem):
        pltpu.make_async_copy(ref, ref, sem).wait()

    def both_copy(r):
        return rank_copy(bsrc, ball.at[t], b_send, b_recv, r)

    def block_rows(outer, b):
        return outer * Z + b

    def ag_copy(b, c, send, where, own=False):
        return pltpu.make_async_remote_copy(
            src_ref=attn.at[:, strip(c)] if own else attn_all.at[block_rows(o, b), c],
            dst_ref=attn_all.at[block_rows(o, b), c],
            send_sem=send,
            recv_sem=ag_recv.at[o, b, c],
            device_id=where,
            device_id_type=MESH,
        )

    def right_copy(s, c):
        return ag_copy((p + Z - s) % Z, c, ag_right.at[s], (o, (p + 1) % Z, t), s == 0)

    def left_copy(s, c):
        return ag_copy((p + s) % Z, c, ag_left.at[s], (o, (p + Z - 1) % Z, t), s == 0)

    def right_sends(s):
        return (p >= s) & (p < Z - 1)

    def left_sends(s):
        return (p + s < Z) & (p > 0)

    def out_copy(b, e, c):
        return ag_copy(b, c, ag_out.at[e], ((o + e) % O, p, t))

    def arrived(outer, b, c):
        rows = attn_all.at[block_rows(outer, b), c]
        return pltpu.make_async_remote_copy(
            src_ref=rows,
            dst_ref=rows,
            send_sem=ag_out.at[0],
            recv_sem=ag_recv.at[outer, b, c],
            device_id=(o, (p + 1) % Z, t),
            device_id_type=MESH,
        )

    def arrival(s, c, ends=False):
        for ok, b in ((p - 1 - s >= 0, (p + Z - 1 - s) % Z), (p + 1 + s < Z, (p + 1 + s) % Z)):

            @pl.when(ok)
            def _():
                arrived(o, b, c).wait_recv()
                for e in range(1, O):
                    out_copy(b, e, c).start()

        if s + 1 < Z - 1:
            for ok, copy in relays(s + 1, ends):

                @pl.when(ok)
                def _():
                    copy(s + 1, c).start()

    def relays(s, ends=False, inner=False):
        right, left = right_sends(s), left_sends(s)
        if ends:
            right, left = right & (p + 2 == Z), left & (p == 1)
        if inner:
            right, left = right & (p + 2 < Z), left & (p > 1)
        return (right, right_copy), (left, left_copy)

    def arrivals(s, first, last, ends=False):
        def one(c, carry):
            arrival(s, c, ends)
            return carry

        lax.fori_loop(first, last, one, 0)

    for ok, copy in ((right_sends(0), right_copy), (left_sends(0), left_copy)):

        @pl.when(ok)
        def _():
            for c in range(strips):
                copy(0, c).start()

    lanes = gain_in.shape[1]
    for c in range(feats // lanes):
        gain[:, c * lanes : (c + 1) * lanes] = gain_in[c : c + 1, :].astype(F32)
        headv[:, c * lanes : (c + 1) * lanes] = head_in[c : c + 1, :].astype(F32)
    both = gain[...] * headv[...]
    for r in range(T):
        for s in range(2):
            for b in range(R):
                start = b * blk + r * q + s * h
                bsrc[r * 2 + s, 0:1, b * h : (b + 1) * h] = both[:, start : start + h]
    ball[t] = bsrc[...]
    valid = pair_valid[...].astype(F32)
    csrc[...] = jnp.broadcast_to(jnp.sum(valid, axis=1, keepdims=True), csrc.shape)

    for r in range(1, T):
        both_copy(r).start()
    for d in range(1, N):
        peer_copy(csrc, cin, c_send, c_recv, d).start()
    for c in range(strips):
        own_copy(c).wait()
        for e in range(1, O):
            out_copy(p, e, c).start()
    for i in range(1, min(SLOTS - 1, steps)):
        load(i).start()

    def turn_attn(x, carry):
        rows = pl.ds(pl.multiple_of(x * 128, 128), 128)
        per = wide // 128
        cols = pl.ds(pl.multiple_of((x % per) * 128, 128), 128)
        attn_t[rows, :] = attn_all[me, x // per, :, cols].T
        return carry

    lax.fori_loop(0, attn.shape[1] // 128, turn_attn, 0)
    resid_copy.wait()

    if h % 128 > 0:

        def turn_resid(c, carry):
            cols = pl.ds(pl.multiple_of(c * 128, 128), 128)
            res_t[cols, :] = res_v[:, cols].T
            return carry

        lax.fori_loop(0, feats // 128, turn_resid, 0)

    hacc[...] = jnp.zeros_like(hacc)

    def rs_copy(s, j, g, mask):
        return pltpu.make_async_remote_copy(
            src_ref=part.at[s, j, g],
            dst_ref=got.at[s, j, g],
            send_sem=rs_send,
            recv_sem=rs_recv.at[s, j - 1, g],
            device_id=rank(flip(t, mask, bits)),
            device_id_type=MESH,
        )

    def rs_mask(s, b):
        return s * 2**b + (1 - s) * 2 ** (bits - 1 - b)

    row16 = lax.broadcasted_iota(jnp.int32, (16, R * h), 0)

    def thirds(row):
        first = row.astype(BF16).astype(F32)
        second = (row - first).astype(BF16).astype(F32)
        third = row - first - second
        rows = jnp.where(row16 == 0, first, jnp.where(row16 == 1, second, third))
        return jnp.where(row16 < 3, rows, 0.0).astype(BF16)

    def add_heads(i):
        s, j, g = piece_of(i)
        r = target(s, j)
        total = hacc[...]
        for n in range(half):
            lhs = thirds(ball[g * half + n, r * 2 + s])
            rows = vbuf[i % 2, n * R * h : (n + 1) * R * h, :]
            high = rows.astype(BF16)
            low = (rows - high.astype(F32)).astype(BF16)
            total = total + jnp.dot(lhs, high, preferred_element_type=F32)
            total = total + jnp.dot(lhs, low, preferred_element_type=F32)
        hacc[...] = total

    def project(i, carry):
        @pl.when(i + SLOTS - 1 < steps)
        def _():
            load(i + SLOTS - 1).start()

        load(i).wait()
        s, j, g = piece_of(i)
        r = target(s, j)
        now = vbuf.at[i % 2]
        now[...] = jnp.dot(
            wbuf[i % SLOTS].reshape(K, wbuf.shape[3]), attn_t[...], preferred_element_type=F32
        )

        @pl.when(t // half == g)
        def _():
            for b in range(R):
                rows = pl.ds(pl.multiple_of(((t % half) * R + b) * h, h), h)
                mine = pl.ds(pl.multiple_of(b * blk + (r * 2 + s) * h, h), h)
                if h % 128 > 0:
                    extra = res_t[mine, :].astype(F32)
                else:
                    extra = res_v[:, mine].astype(F32).T
                now[rows, :] = now[rows, :] + extra

        @pl.when(j >= half)
        def _():
            part[s, j, g] = encode(now[...])
            rs_copy(s, j, g, rs_mask(s, bits - 1)).start()

        @pl.when(j < half)
        def _():
            keep[s, j % half, g] = now[...]

        @pl.when(i == 1)
        def _():
            wait_all(ball.at[pl.ds(0, T - 1)], b_recv)

        @pl.when(i >= 1)
        def _():
            add_heads(i - 1)

        return carry

    lax.fori_loop(0, steps, project, 0)
    add_heads(steps - 1)

    for b in range(bits - 2, -1, -1):

        def combine(x, carry, b=b):
            j, s, g = 2**b + x // 4, x % 2, (x // 2) % 2
            total = keep[s, j, g]
            for up in range(b + 1, bits):
                rs_copy(s, j + 2**up, g, rs_mask(s, up)).wait_recv()
                total = total + decode(got[s, j + 2**up, g])
            part[s, j, g] = encode(total)
            rs_copy(s, j, g, rs_mask(s, b)).start()
            return carry

        lax.fori_loop(0, 4 * 2**b, combine, 0)

    early = max(1, strips - 1)
    arrivals(0, 0, early)
    arrivals(0, early, strips, True)

    def clear(j, carry):
        grad[pl.ds(pl.multiple_of(j * 128, 128), 128), :] = jnp.zeros((128, grad.shape[1]), F32)
        return carry

    lax.fori_loop(0, blk // 128, clear, 0)
    span = R * h
    diag = lax.broadcasted_iota(jnp.int32, (span, span), 0) == lax.broadcasted_iota(
        jnp.int32, (span, span), 1
    )

    def columns(x, carry):
        s, n = x % 2, x // 2
        row = jnp.broadcast_to(ball[n, t * 2 + s], (span, span))
        col = jnp.sum(jnp.where(diag, row, 0.0), axis=1, keepdims=True)
        rows = pl.ds(pl.multiple_of((n % half) * span, span), span)
        bcol[s, n // half, rows, :] = jnp.broadcast_to(col, (span, 128))
        return carry

    lax.fori_loop(0, 2 * T, columns, 0)

    S = lengths.shape[1]
    lens = lengths[...].astype(F32)
    same = lax.broadcasted_iota(jnp.int32, (S, S), 0) == lax.broadcasted_iota(jnp.int32, (S, S), 1)
    lens = jnp.sum(jnp.where(same, jnp.broadcast_to(lens, (S, S)), 0.0), axis=1, keepdims=True)
    seq_len = tok // S
    slot = lax.broadcasted_iota(jnp.int32, (S, tok), 1) - seq_len * lax.broadcasted_iota(
        jnp.int32, (S, tok), 0
    )
    live = (slot >= 0) & (slot.astype(F32) < lens)
    pool = jnp.where(live, 1.0 / lens, 0.0)
    who = lax.broadcasted_iota(jnp.int32, (S, pairs.shape[1]), 0)
    select = jnp.where(who == pairs[0:1, :], 1.0, 0.0) - jnp.where(who == pairs[1:2, :], 1.0, 0.0)

    def final(x, squares):
        s, g = x % 2, x // 2
        total = keep[s, 0, g]
        for up in range(bits - 1, -1, -1):
            rs_copy(s, 2**up, g, rs_mask(s, up)).wait_recv()
            total = total + decode(got[s, 2**up, g])
        keep[s, 0, g] = total
        return squares + jnp.sum(total * total, axis=0, keepdims=True)

    squares = lax.fori_loop(0, 4, final, jnp.zeros((1, tok), F32))
    heads = jnp.sum(hacc[...], axis=0, keepdims=True)
    stat[0:1, :] = squares
    stat[1:2, :] = heads

    def stat_copy(r):
        return rank_copy(stat, stat_in.at[r], st_send, st_recv, r)

    for r in range(1, T):
        stat_copy(r).start()
    count = csrc[0:1, 0:1]
    wait_all(cin.at[pl.ds(1, N - 1)], c_recv)
    for d in range(1, N):
        count = count + cin[d, 0:1, 0:1]
    wait_all(stat_in.at[pl.ds(1, T - 1)], st_recv)
    for r in range(1, T):
        squares = squares + stat_in[r, 0:1, :]
        heads = heads + stat_in[r, 1:2, :]
    inv = 1.0 / jnp.sqrt(squares / width + 1e-05)
    score = heads * inv
    reward = jnp.sum(pool * score, axis=1, keepdims=True)
    margin = jnp.sum(select * reward, axis=0, keepdims=True)
    soft = jnp.maximum(-margin, 0.0) + jnp.log1p(jnp.exp(-jnp.abs(margin)))
    loss = jnp.sum(valid * soft, axis=1, keepdims=True)
    dmargin = -loss_scale[...] * valid * jax.nn.sigmoid(-margin) / count
    dreward = jnp.sum(select * dmargin, axis=1, keepdims=True)
    dscore = jnp.sum(pool * dreward, axis=0, keepdims=True)
    scale = inv * dscore
    pull = inv * inv * inv * dscore * heads / width

    def make_dproj(x, carry):
        s, g, n = x % 2, x // N, (x // 2) % (N // 2)
        rows = pl.ds(pl.multiple_of(n * h, h), h)
        spot = pl.ds(pl.multiple_of(s * h, h), h)
        for c in range(tok // 128):
            cols = slice(c * 128, (c + 1) * 128)
            dp[g * (N // 2) + n, spot, cols] = (
                scale[:, cols] * bcol[s, g, rows, :] - keep[s, 0, g, rows, cols] * pull[:, cols]
            ).astype(BF16)
        return carry

    lax.fori_loop(0, 2 * N, make_dproj, 0)

    side = p // (Z - Z // 2)
    edge = side * (Z - 1 - p) + (1 - side) * p

    def place(i):
        n = i // O
        past = (n + Z - 1 - edge) // Z
        spot = past * n + (1 - past) * (edge - n)
        return ((o + i) % O) * Z + side * (Z - 1 - spot) + (1 - side) * spot

    def slot_rows(r):
        return pl.ds(pl.multiple_of(r * q, q), q)

    def piece_copy(k):
        return pltpu.make_async_remote_copy(
            src_ref=dp.at[k],
            dst_ref=exch.at[me, slot_rows(t)],
            send_sem=z_send,
            recv_sem=z_recv.at[me],
            device_id=replica(k),
            device_id_type=MESH,
        )

    def piece_arrived(k):
        rows = exch.at[k, slot_rows(t)]
        return pltpu.make_async_remote_copy(
            src_ref=rows,
            dst_ref=rows,
            send_sem=z_send,
            recv_sem=z_recv.at[k],
            device_id=replica((me + 1) % N),
            device_id_type=MESH,
        )

    own_piece = pltpu.make_async_copy(dp.at[me], exch.at[me, slot_rows(t)], z_recv.at[me])
    own_piece.start()

    def send_piece(i, carry):
        piece_copy(place(i)).start()
        return carry

    lax.fori_loop(1, N // 2, send_piece, 0)

    @pl.when(edge > 0)
    def _():
        lax.fori_loop(N // 2, N, send_piece, 0)


    lsrc[...] = jnp.broadcast_to(loss, lsrc.shape)
    for s in range(2):
        for g in range(2):
            zw = keep[s, 0, g] * scale
            lanes = zw[:, 0:128]
            for c in range(1, tok // 128):
                lanes = lanes + zw[:, c * 128 : (c + 1) * 128]
            qsrc[s * 2 + g] = jnp.sum(lanes.T, axis=0, keepdims=True)
    for d in range(1, N):
        peer_copy(lsrc, lin, l_send, l_recv, d).start()
        peer_copy(qsrc, qin, q_send, q_recv, d).start()
    for c in range(early, strips):
        for ok, copy in relays(1, inner=True):

            @pl.when(ok)
            def _():
                copy(1, c).start()


    def ag_mask(s, b):
        return 2**b if s == 0 else 2 ** (bits - 1 - b)

    def held(s, c):
        return flip(t, c if s == 0 else reverse(c, bits), bits)

    def half_rows(r, s):
        return pl.ds(pl.multiple_of((r * 2 + s) * h, h), h)

    def spread_copy(k, s, c, b):
        rows = exch.at[k, half_rows(held(s, c), s)]
        return pltpu.make_async_remote_copy(
            src_ref=rows,
            dst_ref=rows,
            send_sem=e_send,
            recv_sem=e_recv.at[k, b],
            device_id=rank(flip(t, ag_mask(s, b), bits)),
            device_id_type=MESH,
        )

    def spread_arrived(k, b):
        wait_all(exch.at[k, pl.ds(0, q * 2**b)], e_recv.at[k, b])

    def begin(i):
        k = place(i)

        @pl.when(k == me)
        def _():
            own_piece.wait()

        @pl.when(k != me)
        def _():
            piece_arrived(k).wait_recv()

        for b in range(bits):
            for s in range(2):
                spread_copy(k, s, 0, b).start()

    def relay(i):
        k = place(i)
        for b in range(bits - 1):
            spread_arrived(k, b)
            for c in range(2**b, 2 ** (b + 1)):
                for s in range(2):
                    for up in range(b + 1, bits):
                        spread_copy(k, s, c, up).start()

    def add_dot(k, c):
        grad[:, strip(c)] += jnp.dot(exch[k], attn_all[k, c], preferred_element_type=F32)

    def rows_ready(k):
        spread_arrived(k, bits - 1)

    def multiply(i):
        k = place(i)
        rows_ready(k)

        def one(c, carry):
            @pl.when(k // Z != o)
            def _():
                arrived(k // Z, k % Z, c).wait_recv()

            add_dot(k, c)
            return carry

        lax.fori_loop(0, strips, one, 0)

    def last_strips(c, carry):
        @pl.when(c < strips)
        def _():
            arrival(Z - 2, c)
            add_dot(place(N - O), c)

        @pl.when(c > 0)
        def _():
            for e in range(1, O):
                k = place(N - O + e)
                arrived(k // Z, k % Z, c - 1).wait_recv()
                add_dot(k, c - 1)

        return carry

    def gather_q():
        total = qsrc[...]
        wait_all(qin.at[pl.ds(1, N - 1)], q_recv)
        for d in range(1, N):
            total = total + qin[d]
        qsum[...] = total
        qall[t] = total
        for r in range(1, T):
            rank_copy(qsum, qall.at[t], t_send, t_recv, r).start()

    def finish_q():
        ltotal = lsrc[...]
        wait_all(lin.at[pl.ds(1, N - 1)], l_recv)
        for d in range(1, N):
            ltotal = ltotal + lin[d]
        loss_out[...] = ltotal[0:1, 0:1] / count
        wait_all(qall.at[pl.ds(0, T - 1)], t_recv)
        for r in range(T):
            for s in range(2):
                for b in range(R):
                    value = jnp.zeros((1, h), F32)
                    for owner in range(T):
                        n = (owner % half) * R + b
                        row = qall[r, s * 2 + owner // half]
                        value = jnp.where(t == owner, row[:, n * h : (n + 1) * h], value)
                    cols = slice(b * blk + r * q + s * h, b * blk + r * q + (s + 1) * h)
                    ggain[:, cols] = value * headv[:, cols]
                    ghead[:, cols] = value * gain[:, cols]

    def stage(i, carry):
        @pl.when(i < N)
        def _():
            begin(i)

        @pl.when((i == O+1) & (edge == 0))
        def _():
            lax.fori_loop(N // 2, N, send_piece, 0)

        for s in range(1, Z - 2):

            @pl.when(i == (1 if s == 1 else 2 + (s + 1) * O))
            def _():
                arrivals(s, 0, early if s == 1 else strips)

            if s == 1:

                @pl.when(i == 2 + 2 * O)
                def _():
                    arrivals(1, early, strips)

        @pl.when(i >= 1)
        def _():
            relay(i - 1)

        @pl.when(i == N - 2)
        def _():
            gather_q()

        @pl.when(i == N)
        def _():
            finish_q()

        @pl.when((i >= 2) & (i < N + 2 - O))
        def _():
            multiply(i - 2)

        return carry

    lax.fori_loop(0, N + 1, stage, 0)
    for e in range(O):
        rows_ready(place(N - O + e))
    lax.fori_loop(0, strips + 1, last_strips, 0)

    for s in range(Z - 1):
        for ok, sem in ((right_sends(s), ag_right), (left_sends(s), ag_left)):

            @pl.when(ok)
            def _():
                wait_all(attn_all.at[0], sem.at[s])

    for e in range(1, O):
        wait_all(attn_all.at[pl.ds(0, Z)], ag_out.at[e])
    wait_all(cin.at[pl.ds(1, N - 1)], c_send)
    wait_all(lin.at[pl.ds(1, N - 1)], l_send)
    wait_all(qin.at[pl.ds(1, N - 1)], q_send)
    wait_all(ball.at[pl.ds(0, T - 1)], b_send)
    wait_all(stat_in.at[pl.ds(1, T - 1)], st_send)
    wait_all(qall.at[pl.ds(0, T - 1)], t_send)
    wait_all(part.at[:, pl.ds(1, T - 1)], rs_send)
    wait_all(dp.at[pl.ds(0, N - 1)], z_send)
    wait_all(exch.at[:, pl.ds(0, (T - 1) * q)], e_send)


def write_out(grad, ggain, ghead, loss, grad_o, ggain_o, ghead_o, loss_o, sems):
    rows = grad.shape[0] // PARTS
    copies = []
    for i in range(PARTS):
        part = pl.ds(i * rows, rows)
        copies.append(pltpu.make_async_copy(grad.at[part], grad_o.at[part], sems.at[i]))
    for i, (src, dst) in enumerate(((ggain, ggain_o), (ghead, ghead_o), (loss, loss_o))):
        copies.append(pltpu.make_async_copy(src, dst, sems.at[PARTS + i]))
    for copy in copies:
        copy.start()
    for copy in copies:
        copy.wait()


def shards(sizes, attn, out_weight, resid, norm_gain, head, lengths, pairs, pair_valid, loss_scale):
    T, O, Z = sizes
    N = O * Z
    tok, feats = resid.shape
    width = feats * T
    blk = width // N
    q = blk // T
    h = q // 2
    K = (N // 2) * h
    R = N // T
    heads_dev = attn.shape[1]
    strips = heads_dev // min(512, heads_dev)
    vmem = pl.BlockSpec(memory_space=pltpu.VMEM)
    anyw = pl.BlockSpec(memory_space=pl.ANY)
    sem = pltpu.SemaphoreType.DMA
    bits = bits_of(T)
    results = pl.pallas_call(
        functools.partial(kernel, sizes),
        out_shape=(
            pltpu.VMEM((blk, heads_dev), F32),
            pltpu.VMEM((1, feats), F32),
            pltpu.VMEM((1, feats), F32),
            pltpu.VMEM((1, 1), F32),
        ),
        in_specs=[anyw] * 3 + [vmem] * 6,
        out_specs=(vmem, vmem, vmem, vmem),
        scratch_shapes=[
            pltpu.VMEM((N, blk, tok), BF16),
            pltpu.VMEM((N, strips, tok, heads_dev // strips), BF16),
            pltpu.VMEM((SLOTS, N // 2, h, heads_dev), BF16),
            pltpu.VMEM((heads_dev, tok), BF16),
            pltpu.VMEM((tok, feats), BF16),
            pltpu.VMEM((feats, tok), BF16),
            pltpu.VMEM((1, feats), F32),
            pltpu.VMEM((1, feats), F32),
            pltpu.VMEM((2, K, tok), F32),
            pltpu.VMEM((2, T, 2, K, tok), BF16),
            pltpu.VMEM((2, T, 2, K, tok), BF16),
            pltpu.VMEM((2, T // 2, 2, K, tok), F32),
            pltpu.VMEM((N, q, tok), BF16),
            pltpu.VMEM((2 * T, 1, R * h), F32),
            pltpu.VMEM((T, 2 * T, 1, R * h), F32),
            pltpu.VMEM((2, 2, K, 128), F32),
            pltpu.VMEM((16, tok), F32),
            pltpu.VMEM((2, tok), F32),
            pltpu.VMEM((T, 2, tok), F32),
            pltpu.VMEM((8, 128), F32),
            pltpu.VMEM((N, 8, 128), F32),
            pltpu.VMEM((8, 128), F32),
            pltpu.VMEM((N, 8, 128), F32),
            pltpu.VMEM((4, 1, K), F32),
            pltpu.VMEM((N, 4, 1, K), F32),
            pltpu.VMEM((4, 1, K), F32),
            pltpu.VMEM((T, 4, 1, K), F32),
            sem((SLOTS,)),
            sem,
            sem((2, T - 1, 2)),
            sem,
            sem,
            sem,
            sem,
            sem,
            sem,
            sem,
            sem,
            sem,
            sem,
            sem,
            sem,
            sem((strips,)),
            sem,
            sem((Z,)),
            sem((Z,)),
            sem((O,)),
            sem((O, Z, strips)),
            sem,
            sem((N,)),
            sem,
            sem((N, bits)),
        ],
        compiler_params=pltpu.CompilerParams(
            collective_id=0, has_side_effects=True, vmem_limit_bytes=50 * 1024 * 1024
        ),
    )(
        attn,
        out_weight.reshape(N, 2 * T, h, heads_dev),
        resid,
        norm_gain.reshape(feats // 128, 128),
        head.reshape(feats // 128, 128),
        lengths[None, :],
        pairs.T,
        pair_valid[None, :],
        loss_scale[None, :],
    )
    grad_out_proj, grad_gain, grad_head, loss = pl.pallas_call(
        write_out,
        out_shape=(
            jax.ShapeDtypeStruct((blk, heads_dev), F32),
            jax.ShapeDtypeStruct((1, feats), F32),
            jax.ShapeDtypeStruct((1, feats), F32),
            jax.ShapeDtypeStruct((1, 1), F32),
        ),
        in_specs=[anyw] * 4,
        out_specs=(anyw,) * 4,
        scratch_shapes=[sem((PARTS + 3,))],
        compiler_params=pltpu.CompilerParams(vmem_limit_bytes=1024 * 1024),
    )(*results)
    return (loss.reshape(1), grad_out_proj, grad_gain[0], grad_head[0])


def solution(mesh):
    sizes = (mesh.shape["tensor"], mesh.shape["outer"], mesh.shape["dp"])
    return jax.shard_map(
        functools.partial(shards, sizes),
        mesh=mesh,
        in_specs=(
            P(("outer", "dp"), "tensor"),
            P(None, "tensor"),
            P(("outer", "dp"), "tensor"),
            P("tensor"),
            P("tensor"),
            P(("outer", "dp")),
            P(("outer", "dp"), None),
            P(("outer", "dp")),
            P(),
        ),
        out_specs=(P(), P(("outer", "dp"), "tensor"), P("tensor"), P("tensor")),
        check_vma=False,
    )
```
